128 devices in a mesh: batch: 1, graph: 128 (over z, y, x, core).
Axes of the slice: x: 4, y: 4, z: 4, core: 2. Of those that a mesh axis runs over, the one named last changes fastest.
Arguments:
- grid_in: float32 [65536, 186], P(('batch', 'graph'))
- mesh_in: float32 [32768, 3], P(('batch', 'graph'))
- edge_in: float32 [1048576, 4], P(('batch', 'graph'))
- edge_src: int32 [1048576], P(('batch', 'graph'))
- edge_dst: int32 [1048576], P(('batch', 'graph'))
- edge_mask: int32 [1048576], P(('batch', 'graph'))
- grid_w1: bfloat16 [186, 512], replicated
- grid_w2: bfloat16 [512, 512], replicated
- grid_vec: float32 [4, 512], replicated
- mesh_w1: bfloat16 [3, 512], replicated
- mesh_w2: bfloat16 [512, 512], replicated
- mesh_vec: float32 [4, 512], replicated
- embed_w1: bfloat16 [4, 512], replicated
- embed_w2: bfloat16 [512, 512], replicated
- embed_vec: float32 [4, 512], replicated
- edge_w1: bfloat16 [1536, 512], replicated
- edge_w2: bfloat16 [512, 512], replicated
- edge_vec: float32 [4, 512], replicated
- node_w1: bfloat16 [1024, 512], replicated
- node_w2: bfloat16 [512, 512], replicated
- node_vec: float32 [4, 512], replicated
- post_w1: bfloat16 [512, 512], replicated
- post_w2: bfloat16 [512, 512], replicated
- post_vec: float32 [4, 512], replicated
- cot_mesh: bfloat16 [32768, 512], P(('batch', 'graph'))
- cot_grid: bfloat16 [65536, 512], P(('batch', 'graph'))
Outputs:
- output 1: bfloat16 [32768, 512], P(('batch', 'graph'))
- output 2: bfloat16 [65536, 512], P(('batch', 'graph'))
- output 3: float32 [65536, 186], P(('batch', 'graph'))
- output 4: float32 [1536, 512], P(('batch', 'graph'))
- output 5: float32 [512, 512], P(('batch', 'graph'))
All inputs are finite; a program needn't handle non-finite values.
Results may differ from the reference program's by a relative error of at most 0.00869367.
Values are sent between devices in bfloat16 or wider.
A program may use at most 1 GiB of HBM per device.

```python
import jax
import jax.numpy as jnp
from jax import lax

GROUP_SIZE = 128
GRID_DEV = 512
MESH_DEV = 256
EDGE_DEV = 8192
LATENT = 512
GRID_FEAT = 186
MESH_FEAT = 3
EDGE_FEAT = 4

NORM_EPS = 1e-5
HALO_ROWS = GRID_DEV // 4
GRID_ROWS = GROUP_SIZE * GRID_DEV
MESH_ROWS = GROUP_SIZE * MESH_DEV
EDGE_ROWS = GROUP_SIZE * EDGE_DEV
AGG_SCALE = max(EDGE_DEV // MESH_DEV, 1) ** -0.5


def draw_graph(graph_key):
    sub_keys = jax.random.split(graph_key, 8)
    band_idx = jnp.arange(GROUP_SIZE)[:, None]
    edge_col = jnp.arange(EDGE_DEV)[None, :]
    cut_pct = jax.random.randint(sub_keys[0], (GROUP_SIZE, 1), 20, 61)
    keep_pct = jax.random.randint(sub_keys[1], (GROUP_SIZE, 1), 25, 101)
    roll_pct = jax.random.randint(sub_keys[2], (GROUP_SIZE, EDGE_DEV), 0, 100)
    local_off = jax.random.randint(sub_keys[3], (GROUP_SIZE, EDGE_DEV), 0, GRID_DEV)
    halo_off = jax.random.randint(sub_keys[4], (GROUP_SIZE, EDGE_DEV), 0, HALO_ROWS)
    take_low = (roll_pct < cut_pct // 2) & (band_idx > 0)
    take_high = (roll_pct >= cut_pct // 2) & (roll_pct < cut_pct) & (band_idx < GROUP_SIZE - 1)
    src_ids = jnp.where(take_low, band_idx * GRID_DEV - 1 - halo_off,
                        jnp.where(take_high, (band_idx + 1) * GRID_DEV + halo_off, band_idx * GRID_DEV + local_off))
    low_end = jnp.maximum(band_idx * GRID_DEV - HALO_ROWS, 0)
    high_end = jnp.minimum((band_idx + 1) * GRID_DEV + HALO_ROWS, GRID_ROWS) - 1
    src_ids = jnp.where(edge_col == 0, low_end, jnp.where(edge_col == 1, high_end, src_ids))
    shift_by = jax.random.randint(sub_keys[5], (GROUP_SIZE, 1), 0, MESH_DEV)
    rand_dst = jax.random.randint(sub_keys[6], (GROUP_SIZE, EDGE_DEV), 0, MESH_DEV)
    dst_ids = jnp.where(edge_col < MESH_DEV, (edge_col + shift_by) % MESH_DEV, rand_dst)
    keep_flag = (jax.random.randint(sub_keys[7], (GROUP_SIZE, EDGE_DEV), 0, 100) < keep_pct) | (edge_col < 2)
    return (src_ids.reshape(EDGE_ROWS).astype(jnp.int32),
            dst_ids.reshape(EDGE_ROWS).astype(jnp.int32),
            keep_flag.reshape(EDGE_ROWS).astype(jnp.int32))


def draw_mlp(mlp_key, fan_in, row_scale):
    sub_keys = jax.random.split(mlp_key, 3)
    w_one = jax.random.normal(sub_keys[0], (fan_in, LATENT), jnp.float32) * row_scale * fan_in ** -0.5
    w_two = jax.random.normal(sub_keys[1], (LATENT, LATENT), jnp.float32) * LATENT ** -0.5
    vec_rows = 0.3 * jax.random.normal(sub_keys[2], (4, LATENT), jnp.float32) + jnp.array([[0.0], [0.0], [1.0], [0.0]], jnp.float32)
    return w_one.astype(jnp.bfloat16), w_two.astype(jnp.bfloat16), vec_rows


def setup_inputs(seed: int = 0, part: int = 0) -> dict:
    root_key = jax.random.key(seed)
    part_key = jax.random.fold_in(root_key, part)
    data_keys = jax.random.split(part_key, 8)
    weight_keys = jax.random.split(jax.random.key(seed + 1), 6)
    lat_pos = (jnp.arange(GRID_ROWS, dtype=jnp.float32) + 0.5) / GRID_ROWS
    freq_rows = jax.random.randint(data_keys[0], (GRID_FEAT,), 1, 9).astype(jnp.float32)
    phase_rows = jax.random.uniform(data_keys[1], (GRID_FEAT,), jnp.float32, 0.0, 6.2832)
    grid_in = jax.random.normal(data_keys[2], (GRID_ROWS, GRID_FEAT), jnp.float32) + 1.5 * jnp.cos(
        jnp.pi * lat_pos[:, None] * freq_rows[None, :] + phase_rows[None, :])
    mesh_in = jax.random.normal(data_keys[3], (MESH_ROWS, MESH_FEAT), jnp.float32)
    edge_in = jax.random.normal(data_keys[4], (EDGE_ROWS, EDGE_FEAT), jnp.float32)
    edge_src, edge_dst, edge_mask = draw_graph(data_keys[5])
    cot_mesh = jax.random.normal(data_keys[6], (MESH_ROWS, LATENT), jnp.float32).astype(jnp.bfloat16)
    cot_grid = (0.25 * jax.random.normal(data_keys[7], (GRID_ROWS, LATENT), jnp.float32)).astype(jnp.bfloat16)
    grid_w1, grid_w2, grid_vec = draw_mlp(weight_keys[0], GRID_FEAT, 1.0)
    mesh_w1, mesh_w2, mesh_vec = draw_mlp(weight_keys[1], MESH_FEAT, 1.0)
    embed_w1, embed_w2, embed_vec = draw_mlp(weight_keys[2], EDGE_FEAT, 1.0)
    edge_w1, edge_w2, edge_vec = draw_mlp(weight_keys[3], 3 * LATENT, 1.0)
    node_scale = jnp.concatenate([jnp.ones((LATENT, 1), jnp.float32), jnp.full((LATENT, 1), AGG_SCALE, jnp.float32)], axis=0)
    node_w1, node_w2, node_vec = draw_mlp(weight_keys[4], 2 * LATENT, node_scale)
    post_w1, post_w2, post_vec = draw_mlp(weight_keys[5], LATENT, 1.0)
    return {'grid_in': grid_in, 'mesh_in': mesh_in, 'edge_in': edge_in, 'edge_src': edge_src, 'edge_dst': edge_dst,
            'edge_mask': edge_mask, 'grid_w1': grid_w1, 'grid_w2': grid_w2, 'grid_vec': grid_vec,
            'mesh_w1': mesh_w1, 'mesh_w2': mesh_w2, 'mesh_vec': mesh_vec, 'embed_w1': embed_w1,
            'embed_w2': embed_w2, 'embed_vec': embed_vec, 'edge_w1': edge_w1, 'edge_w2': edge_w2,
            'edge_vec': edge_vec, 'node_w1': node_w1, 'node_w2': node_w2, 'node_vec': node_vec,
            'post_w1': post_w1, 'post_w2': post_w2, 'post_vec': post_vec, 'cot_mesh': cot_mesh,
            'cot_grid': cot_grid}


def mlp_forward(x_in, w_one, w_two, vec_rows):
    pre_one = jnp.dot(x_in, w_one, preferred_element_type=jnp.float32) + vec_rows[0]
    act_bf = jax.nn.silu(pre_one).astype(jnp.bfloat16)
    pre_two = jnp.dot(act_bf, w_two, preferred_element_type=jnp.float32) + vec_rows[1]
    centred = pre_two - jnp.mean(pre_two, axis=-1, keepdims=True)
    inv_std = lax.rsqrt(jnp.mean(centred * centred, axis=-1, keepdims=True) + NORM_EPS)
    normed = centred * inv_std
    return normed * vec_rows[2] + vec_rows[3], (pre_one, act_bf, normed, inv_std)


def mlp_backward(d_out, w_two, vec_rows, saved_acts):
    pre_one, act_bf, normed, inv_std = saved_acts
    d_norm = d_out * vec_rows[2]
    d_two = inv_std * (d_norm - jnp.mean(d_norm, axis=-1, keepdims=True)
                       - normed * jnp.mean(d_norm * normed, axis=-1, keepdims=True))
    g_two = d_two.astype(jnp.bfloat16)
    d_act = jnp.dot(g_two, w_two.T, preferred_element_type=jnp.float32)
    sig_pre = jax.nn.sigmoid(pre_one)
    d_one = d_act * sig_pre * (1.0 + pre_one * (1.0 - sig_pre))
    return d_one.astype(jnp.bfloat16), g_two


def reference(grid_in, mesh_in, edge_in, edge_src, edge_dst, edge_mask, grid_w1, grid_w2, grid_vec,
              mesh_w1, mesh_w2, mesh_vec, embed_w1, embed_w2, embed_vec, edge_w1, edge_w2, edge_vec,
              node_w1, node_w2, node_vec, post_w1, post_w2, post_vec, cot_mesh, cot_grid):
    grid_y, grid_saved = mlp_forward(grid_in.astype(jnp.bfloat16), grid_w1, grid_w2, grid_vec)
    grid_h = grid_y.astype(jnp.bfloat16)
    post_y, post_saved = mlp_forward(grid_h, post_w1, post_w2, post_vec)
    grid_out = (grid_h.astype(jnp.float32) + post_y).astype(jnp.bfloat16)
    blocks = (mesh_in.reshape(GROUP_SIZE, MESH_DEV, MESH_FEAT),
              edge_in.reshape(GROUP_SIZE, EDGE_DEV, EDGE_FEAT),
              edge_src.reshape(GROUP_SIZE, EDGE_DEV),
              edge_dst.reshape(GROUP_SIZE, EDGE_DEV),
              edge_mask.reshape(GROUP_SIZE, EDGE_DEV),
              cot_mesh.reshape(GROUP_SIZE, MESH_DEV, LATENT))

    def block_step(carry, blk):
        grad_acc, w1_acc, w2_acc = carry
        mesh_blk, edge_blk, src_blk, dst_blk, mask_blk, cot_blk = blk
        mesh_h = mlp_forward(mesh_blk.astype(jnp.bfloat16), mesh_w1, mesh_w2, mesh_vec)[0].astype(jnp.bfloat16)
        edge_h = mlp_forward(edge_blk.astype(jnp.bfloat16), embed_w1, embed_w2, embed_vec)[0].astype(jnp.bfloat16)
        edge_cat = jnp.concatenate([edge_h, grid_h[src_blk], mesh_h[dst_blk]], axis=1)
        edge_y, edge_saved = mlp_forward(edge_cat, edge_w1, edge_w2, edge_vec)
        keep_col = mask_blk.astype(jnp.float32)[:, None]
        message = keep_col * (edge_h.astype(jnp.float32) + edge_y)
        agg_sum = jax.ops.segment_sum(message, dst_blk, num_segments=MESH_DEV).astype(jnp.bfloat16)
        node_y, node_saved = mlp_forward(jnp.concatenate([mesh_h, agg_sum], axis=1), node_w1, node_w2, node_vec)
        mesh_out_blk = (mesh_h.astype(jnp.float32) + node_y).astype(jnp.bfloat16)
        node_g1 = mlp_backward(cot_blk.astype(jnp.float32), node_w2, node_vec, node_saved)[0]
        agg_grad = jnp.dot(node_g1, node_w1[LATENT:].T, preferred_element_type=jnp.float32)
        edge_g1, edge_g2 = mlp_backward(keep_col * agg_grad[dst_blk], edge_w2, edge_vec, edge_saved)
        w1_acc = w1_acc + jnp.dot(edge_cat.T, edge_g1, preferred_element_type=jnp.float32)
        w2_acc = w2_acc + jnp.dot(edge_saved[1].T, edge_g2, preferred_element_type=jnp.float32)
        src_grad = jnp.dot(edge_g1, edge_w1[LATENT:2 * LATENT].T, preferred_element_type=jnp.float32)
        grad_acc = grad_acc.at[src_blk].add(src_grad)
        return (grad_acc, w1_acc, w2_acc), mesh_out_blk

    init_acc = (jnp.zeros((GRID_ROWS, LATENT), jnp.float32), jnp.zeros((3 * LATENT, LATENT), jnp.float32),
                jnp.zeros((LATENT, LATENT), jnp.float32))
    (edge_part, w1_grad, w2_grad), mesh_out = lax.scan(block_step, init_acc, blocks)
    post_g1 = mlp_backward(cot_grid.astype(jnp.float32), post_w2, post_vec, post_saved)[0]
    grid_cot = cot_grid.astype(jnp.float32) + jnp.dot(post_g1, post_w1.T, preferred_element_type=jnp.float32) + edge_part
    grid_g1 = mlp_backward(grid_cot, grid_w2, grid_vec, grid_saved)[0]
    grid_grad = jnp.dot(grid_g1, grid_w1.T, preferred_element_type=jnp.float32)
    return mesh_out.reshape(MESH_ROWS, LATENT), grid_out, grid_grad, w1_grad, w2_grad
```

```python
import functools

import jax
import jax.numpy as jnp
from jax import lax
from jax.experimental import pallas as pl
from jax.experimental.pallas import tpu as pltpu
from jax.sharding import PartitionSpec as P

NORM_EPS = 1e-5
BF = jnp.bfloat16
F32 = jnp.float32
VMEM = pltpu.VMEM
CHUNK = 512


def mlp_forward(x_in, w_one, w_two, vec_rows):
    pre_one = jnp.dot(x_in, w_one, preferred_element_type=F32) + vec_rows[0]
    act_bf = jax.nn.silu(pre_one).astype(BF)
    pre_two = jnp.dot(act_bf, w_two, preferred_element_type=F32) + vec_rows[1]
    centred = pre_two - jnp.mean(pre_two, axis=-1, keepdims=True)
    inv_std = lax.rsqrt(jnp.mean(centred * centred, axis=-1, keepdims=True) + NORM_EPS)
    normed = centred * inv_std
    return normed * vec_rows[2] + vec_rows[3], (pre_one, act_bf, normed, inv_std)


def mlp_backward(d_out, w_two, vec_rows, saved_acts):
    pre_one, act_bf, normed, inv_std = saved_acts
    d_norm = d_out * vec_rows[2]
    d_two = inv_std * (d_norm - jnp.mean(d_norm, axis=-1, keepdims=True)
                       - normed * jnp.mean(d_norm * normed, axis=-1, keepdims=True))
    g_two = d_two.astype(BF)
    d_act = jnp.einsum('nj,kj->nk', g_two, w_two, preferred_element_type=F32)
    sig_pre = jax.nn.sigmoid(pre_one)
    d_one = d_act * sig_pre * (1.0 + pre_one * (1.0 - sig_pre))
    return d_one.astype(BF), g_two


def dot_nn(a, b):
    return jnp.dot(a, b, preferred_element_type=F32)


def dot_nt(a, b):
    return lax.dot_general(a, b, (((1,), (1,)), ((), ())), preferred_element_type=F32)


def dot_tn(a, b):
    return lax.dot_general(a, b, (((0,), (0,)), ((), ())), preferred_element_type=F32)


def split3(x):
    hi = x.astype(BF)
    rest = x - hi.astype(F32)
    mid = rest.astype(BF)
    low = (rest - mid.astype(F32)).astype(BF)
    return hi, mid, low


def silu_bf(p):
    h = 0.5 * p
    return (h + h * jnp.tanh(h)).astype(BF)


def norm_cols(q):
    centred = q - jnp.mean(q, axis=0, keepdims=True)
    inv = lax.rsqrt(jnp.mean(centred * centred, axis=0, keepdims=True) + NORM_EPS)
    return centred * inv, inv


def col(vec_ref, k):
    return vec_ref[:, k:k + 1]


def grad_first(d_act, p):
    t = jnp.tanh(0.5 * p)
    s = 0.5 + 0.5 * t
    return (d_act * (s * (1.0 + p * (1.0 - s)))).astype(BF)


def one_hot(rows, idx):
    return (lax.broadcasted_iota(jnp.int32, (rows, idx.shape[1]), 0) == idx).astype(F32).astype(BF)


def edge_kernel(x_ref, src_ref, dst_ref, dstm_ref, table_ref, hm_ref, cotm_ref, wa_ref, em_w2t_ref, em_vec_ref,
                w1t_ref, w2t_ref, w2_ref, ed_vec_ref, nw1t_ref, nw2t_ref, nd_vec_ref,
                mesh_out_ref, w1g_ref, w2g_ref, tgrad_ref,
                pre_s, norm_s, he_s, inv_s, wl_s, bt_s, agg_s):
    lat = w2_ref.shape[0]
    nt = table_ref.shape[1]
    nm = hm_ref.shape[1]
    steps = pre_s.shape[0]
    ch = pre_s.shape[2]

    wl_s[:, 0:2 * lat] = w1t_ref[:, 0:2 * lat]
    pm = dot_nn(w1t_ref[:, 2 * lat:3 * lat], hm_ref[...]) + col(ed_vec_ref, 0)
    for k, part in enumerate(split3(pm)):
        wl_s[:, 2 * lat + k * nm:2 * lat + (k + 1) * nm] = part
    agg_s[...] = jnp.zeros_like(agg_s)

    def fwd(i, carry):
        sl = pl.ds(pl.multiple_of(i * ch, ch), ch)
        pe = dot_nn(wa_ref[...], x_ref[:, sl])
        ne, _ = norm_cols(dot_nn(em_w2t_ref[...], silu_bf(pe)) + col(em_vec_ref, 1))
        he = (ne * col(em_vec_ref, 2) + col(em_vec_ref, 3)).astype(BF)
        he_s[i] = he
        gath = dot_nn(table_ref[...], one_hot(nt, src_ref[:, sl])).astype(BF)
        ohd = one_hot(nm, dst_ref[:, sl])
        p = dot_nn(wl_s[...], jnp.concatenate([he, gath, ohd, ohd, ohd], axis=0))
        pre_s[i] = p
        n, inv = norm_cols(dot_nn(w2t_ref[...], silu_bf(p)) + col(ed_vec_ref, 1))
        norm_s[i] = n
        inv_s[i] = inv
        msg = he.astype(F32) + (n * col(ed_vec_ref, 2) + col(ed_vec_ref, 3))
        ohm = one_hot(nm, dstm_ref[:, sl])
        agg_s[...] += dot_nt(jnp.concatenate(split3(msg), axis=1), jnp.concatenate([ohm, ohm, ohm], axis=1))
        return carry

    lax.fori_loop(0, steps, fwd, 0)

    hm = hm_ref[...]
    np_ = dot_nn(nw1t_ref[...], jnp.concatenate([hm, agg_s[...].astype(BF)], axis=0)) + col(nd_vec_ref, 0)
    nn_, ninv = norm_cols(dot_nn(nw2t_ref[...], silu_bf(np_)) + col(nd_vec_ref, 1))
    mesh_out_ref[...] = (hm.astype(F32) + (nn_ * col(nd_vec_ref, 2) + col(nd_vec_ref, 3))).astype(BF)
    dn = cotm_ref[...].astype(F32) * col(nd_vec_ref, 2)
    d2 = ninv * (dn - jnp.mean(dn, axis=0, keepdims=True) - nn_ * jnp.mean(dn * nn_, axis=0, keepdims=True))
    ng1 = grad_first(dot_tn(nw2t_ref[...], d2.astype(BF)), np_)
    ag = dot_tn(nw1t_ref[:, lat:2 * lat], ng1) * col(ed_vec_ref, 2)
    ag = ag - jnp.mean(ag, axis=0, keepdims=True)
    for k, part in enumerate(split3(ag)):
        bt_s[:, k * nm:(k + 1) * nm] = part

    w1g_ref[...] = jnp.zeros_like(w1g_ref)
    w2g_ref[...] = jnp.zeros_like(w2g_ref)

    def bwd(i, carry):
        sl = pl.ds(pl.multiple_of(i * ch, ch), ch)
        ohm = one_hot(nm, dstm_ref[:, sl])
        bg = dot_nn(bt_s[...], jnp.concatenate([ohm, ohm, ohm], axis=0))
        n = norm_s[i]
        g2 = (inv_s[i] * (bg - n * jnp.mean(bg * n, axis=0, keepdims=True))).astype(BF)
        p = pre_s[i]
        w2g_ref[...] += dot_nt(silu_bf(p), g2)
        g1 = grad_first(dot_nn(w2_ref[...], g2), p)
        w1g_ref[...] += dot_nt(jnp.concatenate([he_s[i], one_hot(nt, src_ref[:, sl]), ohm], axis=0), g1)
        return carry

    lax.fori_loop(0, steps, bwd, 0)

    sp = split3(w1g_ref[lat:lat + nt, :])
    tp = split3(w1g_ref[lat + nt:lat + nt + nm, :])
    table = table_ref[...]
    w1g_ref[lat:2 * lat, :] = dot_nn(jnp.concatenate([table, table, table], axis=1), jnp.concatenate(sp, axis=0))
    w1g_ref[2 * lat:3 * lat, :] = dot_nn(jnp.concatenate([hm, hm, hm], axis=1),
                                         jnp.concatenate(tp, axis=0))
    wb = w1t_ref[:, lat:2 * lat].T
    tgrad_ref[...] = dot_nt(jnp.concatenate([wb, wb, wb], axis=1), jnp.concatenate(sp, axis=1))


def edge_call(x_aug, src, dst, dstm, table, hm, cotm, wa, em_w2t, em_vec, w1t, w2t, w2, ed_vec,
              nw1t, nw2t, nd_vec):
    lat, nt, nm, edges = w2.shape[0], table.shape[1], hm.shape[1], src.shape[1]
    steps = edges // CHUNK
    out_shape = (jax.ShapeDtypeStruct((lat, nm), BF), jax.ShapeDtypeStruct((3 * lat, lat), F32),
                 jax.ShapeDtypeStruct((lat, lat), F32), jax.ShapeDtypeStruct((lat, nt), F32))
    return pl.pallas_call(
        edge_kernel,
        out_shape=out_shape,
        in_specs=[pl.BlockSpec(memory_space=VMEM)] * 17,
        out_specs=(pl.BlockSpec(memory_space=VMEM),) * 4,
        scratch_shapes=[VMEM((steps, lat, CHUNK), F32), VMEM((steps, lat, CHUNK), F32), VMEM((steps, lat, CHUNK), BF),
                        VMEM((steps, 1, CHUNK), F32), VMEM((lat, 2 * lat + 3 * nm), BF), VMEM((lat, 3 * nm), BF),
                        VMEM((lat, nm), F32)],
        compiler_params=pltpu.CompilerParams(vmem_limit_bytes=67043328),
        name='edge_pass',
    )(x_aug, src, dst, dstm, table, hm, cotm, wa, em_w2t, em_vec, w1t, w2t, w2, ed_vec,
      nw1t, nw2t, nd_vec)


def scatter_kernel(w1_ref, w2_ref, o1_ref, o2_ref,
                   r0a, r0b, r0c, a0, b0, c0, ra1, rb1, rc1, a1, b1, c1, ra2, rb2, rc2, a2, b2, c2, ra3, rb3, rc3,
                   f1, f2, rf1, rf2, send0, recv0, sends, recvs, send4, recv4):
    me = lax.axis_index('graph')
    core = lax.rem(me, 2)
    chip = me // 2
    px, py, pz = lax.rem(chip, 4), lax.rem(chip // 4, 4), chip // 16

    def dev(z, y, x, k):
        return {'graph': ((z * 4 + y) * 4 + x) * 2 + k}

    def turn(v, d):
        return lax.rem(v + d, 4)

    partner = dev(pz, py, px, 1 - core)
    peers = {'x': [dev(pz, py, turn(px, d), core) for d in (1, 2, 3)],
             'y': [dev(pz, turn(py, d), px, core) for d in (1, 2, 3)],
             'z': [dev(turn(pz, d), py, px, core) for d in (1, 2, 3)]}
    pos = {'x': px, 'y': py, 'z': pz}
    barrier = pltpu.get_barrier_semaphore()
    for peer in [partner] + peers['x'] + peers['y'] + peers['z']:
        pl.semaphore_signal(barrier, inc=1, device_id=peer, device_id_type=pl.DeviceIdType.MESH)
    pl.semaphore_wait(barrier, 10)

    half = w1_ref.shape[-1] // 2
    mine = pl.multiple_of(core * half, half)
    his = pl.multiple_of((1 - core) * half, half)
    q = half // 2

    def copy(src, dst, ssem, rsem, peer):
        c = pltpu.make_async_remote_copy(src_ref=src, dst_ref=dst, send_sem=ssem, recv_sem=rsem, device_id=peer,
                                         device_id_type=pl.DeviceIdType.MESH)
        c.start()
        return c

    first = [copy(w1_ref.at[:, :, :, :, pl.ds(his, q)], r0a, send0.at[0], recv0.at[0], partner),
             copy(w1_ref.at[:, :, :, :, pl.ds(pl.multiple_of(his + q, q), q)], r0b, send0.at[1], recv0.at[1], partner),
             copy(w2_ref.at[:, :, :, :, pl.ds(his, half)], r0c, send0.at[2], recv0.at[2], partner)]

    def pick(ref, axis_at, v):
        if axis_at == 0:
            return ref.at[v]
        if axis_at == 1:
            return ref.at[:, v]
        return ref.at[:, :, v]

    plans = {'a': [('x', 2), ('y', 1), ('z', 0)], 'b': [('y', 1), ('z', 0), ('x', 0)],
             'c': [('z', 0), ('x', 1), ('y', 0)]}
    accs = {'a': [a0, a1, a2, f1.at[:, pl.ds(0, q)]], 'b': [b0, b1, b2, f1.at[:, pl.ds(q, q)]], 'c': [c0, c1, c2, f2]}
    bufs = {'a': [ra1, ra2, ra3], 'b': [rb1, rb2, rb3], 'c': [rc1, rc2, rc3]}
    order = ['a', 'b', 'c']

    def launch(name, stage):
        ax, at = plans[name][stage]
        n = order.index(name)
        return [copy(pick(accs[name][stage], at, turn(pos[ax], d)), bufs[name][stage].at[d - 1],
                     sends.at[n, stage, d - 1], recvs.at[n, stage, d - 1], peers[ax][d - 1]) for d in (2, 1, 3)]

    flying = {}
    for n, name in enumerate(order):
        first[n].wait_recv()
        if name == 'a':
            a0[...] = w1_ref[:, :, :, :, pl.ds(mine, q)] + r0a[...]
        elif name == 'b':
            b0[...] = w1_ref[:, :, :, :, pl.ds(pl.multiple_of(mine + q, q), q)] + r0b[...]
        else:
            c0[...] = w2_ref[:, :, :, :, pl.ds(mine, half)] + r0c[...]
        flying[name] = launch(name, 0)
    started = list(first)
    for stage in range(3):
        for name in order:
            for c in flying[name]:
                c.wait_recv()
            started += flying[name]
            ax, at = plans[name][stage]
            rb = bufs[name][stage]
            accs[name][stage + 1][...] = (pick(accs[name][stage], at, pos[ax])[...] + rb[0]) + (rb[1] + rb[2])
            if stage < 2:
                flying[name] = launch(name, stage + 1)

    rows1, rows2 = o1_ref.shape[0], o2_ref.shape[0]
    win = rows1 + rows2
    last = [copy(f1.at[pl.ds(pl.multiple_of((1 - core) * 8, 8), win)], rf1, send4.at[0], recv4.at[0], partner),
            copy(f2, rf2, send4.at[1], recv4.at[1], partner)]
    own1 = f1[pl.ds(pl.multiple_of(core * 8, 8), win), :]
    own2 = f2[...]
    for c in last:
        c.wait_recv()
    low = core == 0
    o1_ref[:, pl.ds(mine, half)] = jnp.where(low, own1[0:rows1], own1[rows2:win])
    o1_ref[:, pl.ds(his, half)] = jnp.where(low, rf1[0:rows1, :], rf1[rows2:win, :])
    o2_ref[:, pl.ds(mine, half)] = jnp.where(low, own2[0:rows2], own2[rows2:2 * rows2])
    o2_ref[:, pl.ds(his, half)] = jnp.where(low, rf2[0:rows2, :], rf2[rows2:2 * rows2, :])
    for c in started + last:
        c.wait_send()


def scatter_call(w1g, w2g):
    r1, r2, cols = w1g.shape[0] // 64, w2g.shape[0] // 64, w1g.shape[1]
    half, q = cols // 2, cols // 4
    dma = pltpu.SemaphoreType.DMA

    def f(*shape):
        return VMEM(shape, F32)

    scratch = [f(4, 4, 4, r1, q), f(4, 4, 4, r1, q), f(4, 4, 4, r2, half),
               f(4, 4, 4, r1, q), f(4, 4, 4, r1, q), f(4, 4, 4, r2, half),
               f(3, 4, 4, r1, q), f(3, 4, 4, r1, q), f(3, 4, 4, r2, half),
               f(4, 4, r1, q), f(4, 4, r1, q), f(4, 4, r2, half),
               f(3, 4, r1, q), f(3, 4, r1, q), f(3, 4, r2, half),
               f(4, r1, q), f(4, r1, q), f(4, r2, half),
               f(3, r1, q), f(3, r1, q), f(3, r2, half),
               f(r1, half), f(r2, half), f(16, half), f(r2, half),
               dma((3,)), dma((3,)), dma((3, 3, 3)), dma((3, 3, 3)), dma((2,)), dma((2,))]
    return pl.pallas_call(
        scatter_kernel,
        out_shape=(jax.ShapeDtypeStruct((r1 // 2, cols), F32), jax.ShapeDtypeStruct((r2 // 2, cols), F32)),
        in_specs=[pl.BlockSpec(memory_space=VMEM)] * 2,
        out_specs=(pl.BlockSpec(memory_space=VMEM),) * 2,
        scratch_shapes=scratch,
        compiler_params=pltpu.CompilerParams(collective_id=0, has_side_effects=True, vmem_limit_bytes=32 << 20),
        name='grad_scatter',
    )(w1g.reshape(4, 4, 4, r1, cols), w2g.reshape(4, 4, 4, r2, cols))


def bias_terms(row):
    hi = lax.reduce_precision(row, 8, 7)
    mid = lax.reduce_precision(row - hi, 8, 7)
    return [hi.astype(BF), mid.astype(BF), (row - hi - mid).astype(BF)]


def solution(mesh):
    groups = mesh.shape['graph']
    row_spec = P(('batch', 'graph'), None)
    flat_spec = P(('batch', 'graph'))
    rep_spec = P(None, None)
    down_perm = [(src_dev, src_dev - 1) for src_dev in range(1, groups)]
    up_perm = [(src_dev, src_dev + 1) for src_dev in range(groups - 1)]

    def device_step(grid_in, mesh_in, edge_in, edge_src, edge_dst, edge_mask, grid_w1, grid_w2, grid_vec,
                    mesh_w1, mesh_w2, mesh_vec, embed_w1, embed_w2, embed_vec, edge_w1, edge_w2, edge_vec,
                    node_w1, node_w2, node_vec, post_w1, post_w2, post_vec, cot_mesh, cot_grid):
        band_rows = grid_in.shape[0]
        halo_rows = band_rows // 4
        latent = grid_w2.shape[1]
        edges = edge_in.shape[0]
        band_index = lax.axis_index('graph')
        grid_y, grid_saved = mlp_forward(grid_in.astype(BF), grid_w1, grid_w2, grid_vec)
        grid_h = grid_y.astype(BF)
        from_above = lax.ppermute(grid_h[:halo_rows], 'graph', down_perm)
        from_below = lax.ppermute(grid_h[band_rows - halo_rows:], 'graph', up_perm)
        row_table = jnp.concatenate([from_below, grid_h, from_above], axis=0)
        local_src = edge_src - (band_index * band_rows - halo_rows)
        mesh_h = mlp_forward(mesh_in.astype(BF), mesh_w1, mesh_w2, mesh_vec)[0].astype(BF)
        x_aug = jnp.concatenate([edge_in.T.astype(BF), jnp.ones((3, edges), BF),
                                 jnp.zeros((9, edges), BF)], axis=0)
        wa = jnp.concatenate([embed_w1.T] + [t[:, None] for t in bias_terms(embed_vec[0])]
                             + [jnp.zeros((latent, 9), BF)], axis=1)
        dstm = jnp.where(edge_mask > 0, edge_dst, -1)
        mesh_out_t, w1_part, w2_part, tgrad_t = edge_call(
            x_aug, local_src[None], edge_dst[None], dstm[None], row_table.T, mesh_h.T, cot_mesh.T, wa,
            embed_w2.T, embed_vec.T, edge_w1.T, edge_w2.T, edge_w2, edge_vec.T,
            node_w1.T, node_w2.T, node_vec.T)
        mesh_out = mesh_out_t.T
        table_grad = tgrad_t.T
        post_y, post_saved = mlp_forward(grid_h, post_w1, post_w2, post_vec)
        grid_out = (grid_h.astype(F32) + post_y).astype(BF)
        tail_grad = lax.ppermute(table_grad[:halo_rows], 'graph', down_perm)
        head_grad = lax.ppermute(table_grad[band_rows + halo_rows:], 'graph', up_perm)
        edge_part = table_grad[halo_rows:band_rows + halo_rows] + jnp.concatenate(
            [head_grad, jnp.zeros((band_rows - 2 * halo_rows, latent), F32), tail_grad], axis=0)
        post_g1 = mlp_backward(cot_grid.astype(F32), post_w2, post_vec, post_saved)[0]
        grid_cot = cot_grid.astype(F32) + jnp.einsum('nj,kj->nk', post_g1, post_w1,
                                                     preferred_element_type=F32) + edge_part
        grid_g1 = mlp_backward(grid_cot, grid_w2, grid_vec, grid_saved)[0]
        grid_grad = jnp.einsum('nj,kj->nk', grid_g1, grid_w1, preferred_element_type=F32)
        w1_grad, w2_grad = scatter_call(w1_part, w2_part)
        return mesh_out, grid_out, grid_grad, w1_grad, w2_grad

    in_specs = (row_spec, row_spec, row_spec, flat_spec, flat_spec, flat_spec) + (rep_spec,) * 18 + (row_spec, row_spec)
    return jax.shard_map(device_step, mesh=mesh, in_specs=in_specs, out_specs=(row_spec,) * 5, check_vma=False)
```

```python
import jax
import jax.numpy as jnp
from jax import lax
from jax.experimental import pallas as pl
from jax.experimental.pallas import tpu as pltpu
from jax.sharding import PartitionSpec as P

NORM_EPS = 1e-5
BF = jnp.bfloat16
F32 = jnp.float32
VMEM = pltpu.VMEM
CHUNK = 512
FETCHED = (10, 13, 15, 21, 22, 25)
DEV = pl.DeviceIdType.MESH
GRID, MESH, EMBED, EDGE, NODE, POST = range(6)


def dot_nn(a, b):
    return jnp.dot(a, b, preferred_element_type=F32)


def dot_nt(a, b):
    return lax.dot_general(a, b, (((1,), (1,)), ((), ())), preferred_element_type=F32)


def dot_tn(a, b):
    return lax.dot_general(a, b, (((0,), (0,)), ((), ())), preferred_element_type=F32)


def split3(x):
    hi = x.astype(BF)
    rest = x - hi.astype(F32)
    mid = rest.astype(BF)
    low = (rest - mid.astype(F32)).astype(BF)
    return [hi, mid, low]


def silu_bf(p):
    h = 0.5 * p
    return (h + h * jnp.tanh(h)).astype(BF)


def norm_cols(q):
    centred = q - jnp.mean(q, axis=0, keepdims=True)
    inv = lax.rsqrt(jnp.mean(centred * centred, axis=0, keepdims=True) + NORM_EPS)
    return centred * inv, inv


def norm_back(d, n, inv):
    return inv * (d - jnp.mean(d, axis=0, keepdims=True) - n * jnp.mean(d * n, axis=0, keepdims=True))


def grad_first(d_act, p):
    t = jnp.tanh(0.5 * p)
    s = 0.5 + 0.5 * t
    return (d_act * (s * (1.0 + p * (1.0 - s)))).astype(BF)


def one_hot(rows, idx):
    return (lax.broadcasted_iota(jnp.int32, (rows, idx.shape[1]), 0) == idx).astype(F32).astype(BF)


def lanes(*parts):
    return jnp.concatenate(parts, axis=1)


def rows(*parts):
    return jnp.concatenate(parts, axis=0)


def step_kernel(gx_ref, mx_ref, ex_ref, src_ref, dst_ref, mask_ref,
                gw1_ref, gw2_ref, gvec_ref, mw1_ref, mw2_ref, mvec_ref, ew1_ref, ew2_ref, evec_ref,
                dw1_ref, dw2_ref, dvec_ref, nw1_ref, nw2_ref, nvec_ref, pw1_ref, pw2_ref, pvec_ref,
                cotm_ref, cotg_ref,
                mesh_out_ref, grid_out_ref, ggrad_ref, o1_ref, o2_ref,
                pre_s, norm_s, he_s, inv_s, wl_s, bt_s, agg_s, w1g_s, w2g_s, table_s, hm_s, ew2t_s, dw2t_s, v_s, vt_s,
                stage_sem, done_sem, hs_sem, hr_sem, ts_sem, tr_sem, send0, recv0, sends, recvs, send4, recv4):
    lat = dw2_ref.shape[0]
    band = gx_ref.shape[1]
    nm = mx_ref.shape[1]
    halo = band // 4
    nt = band + 2 * halo
    ch = he_s.shape[1]
    steps = he_s.shape[0] // lat

    me = lax.axis_index('graph')
    total = 128
    core = lax.rem(me, 2)
    chip = me // 2
    px, py, pz = lax.rem(chip, 4), lax.rem(chip // 4, 4), chip // 16

    def dev(z, y, x, k):
        return {'graph': ((z * 4 + y) * 4 + x) * 2 + k}

    def turn(v, d):
        return lax.rem(v + d, 4)

    below = {'graph': lax.rem(me + total - 1, total)}
    above = {'graph': lax.rem(me + 1, total)}
    partner = dev(pz, py, px, 1 - core)
    peers = {'x': [dev(pz, py, turn(px, d), core) for d in (1, 2, 3)],
             'y': [dev(pz, turn(py, d), px, core) for d in (1, 2, 3)],
             'z': [dev(turn(pz, d), py, px, core) for d in (1, 2, 3)]}
    pos = {'x': px, 'y': py, 'z': pz}
    everyone = [below, above, partner] + peers['x'] + peers['y'] + peers['z']

    def fetch(k, src, slot):
        n = src.shape[0]
        c = pltpu.make_async_copy(src, he_s.at[slot * lat:slot * lat + n, :], stage_sem.at[k])
        c.start()
        return c

    def held(slot, n=1):
        return he_s[slot * lat:(slot + n) * lat, :]

    early = [fetch(0, mw2_ref, 15), fetch(1, dw1_ref, 10), fetch(2, ew2_ref, 14)]

    barrier = pltpu.get_barrier_semaphore()
    for peer in everyone:
        pl.semaphore_signal(barrier, inc=1, device_id=peer, device_id_type=DEV)

    def copy(src, dst, ssem, rsem, peer):
        c = pltpu.make_async_remote_copy(src_ref=src, dst_ref=dst, send_sem=ssem, recv_sem=rsem, device_id=peer,
                                         device_id_type=DEV)
        c.start()
        return c

    v_s[...] = jnp.zeros_like(v_s)
    for k, ref in enumerate((gvec_ref, mvec_ref, evec_ref, dvec_ref, nvec_ref, pvec_ref)):
        v_s[4 * k:4 * k + 4, :] = ref[...]
    vt_s[...] = v_s[...].T

    def col(mlp, k):
        return vt_s[:, 4 * mlp + k:4 * mlp + k + 1]

    def scaled(n, mlp):
        return n * col(mlp, 2) + col(mlp, 3)

    def grid_forward():
        p = dot_tn(gw1_ref[...], gx_ref[...].astype(BF)) + col(GRID, 0)
        n, inv = norm_cols(dot_tn(gw2_ref[...], silu_bf(p)) + col(GRID, 1))
        return p, n, inv

    table_s[:, halo:halo + band] = scaled(grid_forward()[1], GRID).astype(BF)
    pl.semaphore_wait(barrier, len(everyone))
    halos = [copy(table_s.at[:, halo:2 * halo], table_s.at[:, halo + band:nt], hs_sem.at[0], hr_sem.at[0], below),
             copy(table_s.at[:, band:band + halo], table_s.at[:, 0:halo], hs_sem.at[1], hr_sem.at[1], above)]

    for c in early:
        c.wait()
    mp = dot_tn(mw1_ref[...], mx_ref[...].astype(BF)) + col(MESH, 0)
    mn, _ = norm_cols(dot_tn(held(15), silu_bf(mp)) + col(MESH, 1))
    hm_s[...] = scaled(mn, MESH).astype(BF)

    wl_s[:, 0:lat] = held(10).T
    wl_s[:, lat:2 * lat] = held(11).T
    ew2t_s[...] = held(14).T
    dw2t_s[...] = dw2_ref[...].T
    pm = dot_tn(held(12), hm_s[...]) + col(EDGE, 0)
    for k, part in enumerate(split3(pm)):
        wl_s[:, 2 * lat + k * nm:2 * lat + (k + 1) * nm] = part
    agg_s[...] = jnp.zeros_like(agg_s)
    base = me * band - halo

    def slab(i):
        return pl.ds(pl.multiple_of(i * ch, ch), ch)

    def masked_dst(sl):
        return jnp.where(mask_ref[:, sl] > 0, dst_ref[:, sl], -1)

    def embed(i):
        pe = dot_tn(ew1_ref[...], ex_ref[:, slab(i)].astype(BF)) + col(EMBED, 0)
        ne, _ = norm_cols(dot_nn(ew2t_s[...], silu_bf(pe)) + col(EMBED, 1))
        he_s[slab(i), :] = scaled(ne, EMBED).astype(BF)

    def first_half(i):
        sl = slab(i)
        gath = dot_nn(table_s[...], one_hot(nt, src_ref[:, sl] - base)).astype(BF)
        ohd = one_hot(nm, dst_ref[:, sl])
        pre_s[sl, :] = dot_nn(wl_s[...], rows(he_s[sl, :], gath, ohd, ohd, ohd))

    def second_half(i):
        sl = slab(i)
        n, inv = norm_cols(dot_nn(dw2t_s[...], silu_bf(pre_s[sl, :])) + col(EDGE, 1))
        norm_s[sl, :] = n
        inv_s[i] = inv
        msg = he_s[sl, :].astype(F32) + scaled(n, EDGE)
        ohm = one_hot(nm, masked_dst(sl))
        agg_s[...] += dot_nt(lanes(*split3(msg)), lanes(ohm, ohm, ohm))

    def fwd(i, carry):
        second_half(i - 1)
        first_half(i)
        embed(jnp.minimum(i + 1, steps - 1))
        return carry

    embed(0)
    embed(1)
    for c in halos:
        c.wait_recv()
    first_half(0)
    lax.fori_loop(1, steps, fwd, 0)
    second_half(steps - 1)

    hm = hm_s[...]
    np_ = dot_tn(nw1_ref[...], rows(hm, agg_s[...].astype(BF))) + col(NODE, 0)
    nn_, ninv = norm_cols(dot_tn(nw2_ref[...], silu_bf(np_)) + col(NODE, 1))
    mesh_out_ref[...] = (hm.astype(F32) + scaled(nn_, NODE)).T.astype(BF)
    d2 = norm_back(cotm_ref[...].astype(F32).T * col(NODE, 2), nn_, ninv)
    ng1 = grad_first(dot_nn(nw2_ref[...], d2.astype(BF)), np_)
    ag = dot_nn(nw1_ref[lat:2 * lat, :], ng1) * col(EDGE, 2)
    ag = ag - jnp.mean(ag, axis=0, keepdims=True)
    for k, part in enumerate(split3(ag)):
        bt_s[:, k * nm:(k + 1) * nm] = part

    w1g_s[...] = jnp.zeros_like(w1g_s)
    w2g_s[...] = jnp.zeros_like(w2g_s)

    def bwd(i, carry):
        sl = slab(i)
        ohm = one_hot(nm, masked_dst(sl))
        bg = dot_nn(bt_s[...], rows(ohm, ohm, ohm))
        n = norm_s[sl, :]
        g2 = (inv_s[i] * (bg - n * jnp.mean(bg * n, axis=0, keepdims=True))).astype(BF)
        p = pre_s[sl, :]
        w2g_s[...] += dot_nt(silu_bf(p), g2)
        g1 = grad_first(dot_nn(dw2_ref[...], g2), p)
        w1g_s[...] += dot_nt(rows(he_s[sl, :], one_hot(nt, src_ref[:, sl] - base), ohm), g1)
        return carry

    lax.fori_loop(0, steps, bwd, 0)

    for peer in everyone:
        pl.semaphore_signal(done_sem, inc=1, device_id=peer, device_id_type=DEV)
    late = [fetch(3, dw1_ref.at[lat:2 * lat, :], 8), fetch(4, pw1_ref, 5), fetch(5, pw2_ref, 6), fetch(6, cotg_ref, 7)]
    for k, part in enumerate(split3(w1g_s[lat:lat + nt, :])):
        he_s[k * nt:(k + 1) * nt, :] = part
    t0 = 9 * lat
    for k, part in enumerate(split3(w1g_s[lat + nt:lat + nt + nm, :])):
        he_s[t0 + k * nm:t0 + (k + 1) * nm, :] = part
    for c in late:
        c.wait()
    wb = held(8)
    tg = dot_nt(lanes(wb, wb, wb), lanes(he_s[0:nt, :], he_s[nt:2 * nt, :], he_s[2 * nt:3 * nt, :]))
    norm_s[0:lat, 0:halo] = tg[:, 0:halo]
    norm_s[0:lat, halo:2 * halo] = tg[:, halo + band:nt]
    norm_s[lat:2 * lat, :] = tg[:, halo:halo + band]
    pl.semaphore_wait(done_sem, len(everyone))
    tails = [copy(norm_s.at[0:lat, 0:halo], pre_s.at[0:lat, 2 * halo:3 * halo], ts_sem.at[0], tr_sem.at[0], below),
             copy(norm_s.at[0:lat, halo:2 * halo], pre_s.at[0:lat, 3 * halo:4 * halo], ts_sem.at[1], tr_sem.at[1],
                  above)]
    half = lat // 2
    q = half // 2
    mine = pl.multiple_of(core * half, half)
    his = pl.multiple_of((1 - core) * half, half)
    n1, n2 = 3 * lat, lat
    first = {'c': copy(w2g_s.at[:, pl.ds(his, half)], pre_s.at[n1:n1 + n2, 0:half], send0.at[2], recv0.at[2], partner)}
    tb = table_s[...]
    w1g_s[lat:2 * lat, :] = dot_nn(lanes(tb, tb, tb), he_s[0:3 * nt, :])
    w1g_s[2 * lat:3 * lat, :] = dot_nn(lanes(hm, hm, hm), he_s[t0:t0 + 3 * nm, :])
    first['a'] = copy(w1g_s.at[:, pl.ds(his, q)], pre_s.at[0:n1, 0:q], send0.at[0], recv0.at[0], partner)
    first['b'] = copy(w1g_s.at[:, pl.ds(pl.multiple_of(his + q, q), q)], pre_s.at[0:n1, q:half], send0.at[1],
                      recv0.at[1], partner)

    gp, gn, ginv = grid_forward()
    keep_p, keep_n = slice(10 * lat, 11 * lat), slice(11 * lat, 12 * lat)
    norm_s[keep_p, :] = gp
    norm_s[keep_n, :] = gn
    inv_s[0] = ginv
    hg = table_s[:, halo:halo + band]
    pp = dot_tn(held(5), hg) + col(POST, 0)
    pn, pinv = norm_cols(dot_tn(held(6), silu_bf(pp)) + col(POST, 1))
    grid_out_ref[...] = (hg.astype(F32) + scaled(pn, POST)).T.astype(BF)
    cg = held(7).astype(F32).T
    pd = norm_back(cg * col(POST, 2), pn, pinv)
    pg1 = grad_first(dot_nn(held(6), pd.astype(BF)), pp)
    norm_s[2 * lat:3 * lat, :] = cg + dot_nn(held(5), pg1)

    b1, b2 = n1 // 64, n2 // 64
    shape = {'a': (b1, 0, q), 'b': (b1, q, q), 'c': (b2, 0, half)}
    axes = {'a': 'xyz', 'b': 'yzx', 'c': 'zxy'}
    order = 'cab'
    at = {'a': 0, 'b': 0, 'c': 64 * b1}
    acc_rows = {k: [] for k in order}
    buf_rows = {k: [] for k in order}
    top_a, top_b = 4 * lat, n1 + n2
    for stage in range(4):
        for k in 'ac':
            acc_rows[k].append(top_a)
            top_a += shape[k][0] * 4 ** (3 - stage)
            buf_rows[k].append(top_b)
            top_b += 0 if stage == 3 else 3 * shape[k][0] * 4 ** (2 - stage)
    acc_rows['b'], buf_rows['b'] = acc_rows['a'], buf_rows['a']

    def acc_at(k, stage, off, n):
        return norm_s.at[pl.ds(acc_rows[k][stage] + off, n), shape[k][1]:shape[k][1] + shape[k][2]]

    def buf_at(k, stage, slot, n):
        return pre_s.at[pl.ds(buf_rows[k][stage] + slot * n, n), shape[k][1]:shape[k][1] + shape[k][2]]

    def launch(k, stage):
        n = shape[k][0] * 4 ** (2 - stage)
        ax = axes[k][stage]
        j = order.index(k)
        return [copy(acc_at(k, stage, pl.multiple_of(turn(pos[ax], d) * n, 8), n), buf_at(k, stage, d - 1, n),
                     sends.at[j, stage, d - 1], recvs.at[j, stage, d - 1], peers[ax][d - 1]) for d in (2, 1, 3)]

    flying = {}
    for k in order:
        n, c0, w = shape[k]
        first[k].wait_recv()
        src = w2g_s if k == 'c' else w1g_s
        for i in range(64):
            v = {'z': i // 16, 'y': i // 4 % 4, 'x': i % 4}
            to = (v[axes[k][0]] * 4 + v[axes[k][1]]) * 4 + v[axes[k][2]]
            acc_at(k, 0, to * n, n)[...] = (src[i * n:(i + 1) * n, pl.ds(pl.multiple_of(mine + c0, q), w)]
                                            + pre_s[at[k] + i * n:at[k] + (i + 1) * n, c0:c0 + w])
        flying[k] = launch(k, 0)
    started = tails + halos + [first[k] for k in order]

    for c in tails:
        c.wait_recv()
    own = norm_s[2 * lat:3 * lat, :] + norm_s[lat:2 * lat, :]
    ends = lanes(own[:, 0:halo] + pre_s[0:lat, 3 * halo:4 * halo], own[:, halo:band - halo],
                 own[:, band - halo:band] + pre_s[0:lat, 2 * halo:3 * halo])
    gd = norm_back(ends * col(GRID, 2), norm_s[keep_n, :], inv_s[0])
    gg1 = grad_first(dot_nn(gw2_ref[...], gd.astype(BF)), norm_s[keep_p, :])
    ggrad_ref[...] = dot_nn(gw1_ref[...], gg1)

    for stage in range(3):
        for k in order:
            for c in flying[k]:
                c.wait_recv()
            started += flying[k]
            n = shape[k][0] * 4 ** (2 - stage)
            keep = acc_at(k, stage, pl.multiple_of(pos[axes[k][stage]] * n, 8), n)[...]
            acc_at(k, stage + 1, 0, n)[...] = (keep + buf_at(k, stage, 0, n)[...]) + (
                buf_at(k, stage, 1, n)[...] + buf_at(k, stage, 2, n)[...])
            if stage < 2:
                flying[k] = launch(k, stage + 1)

    r1, r2 = o1_ref.shape[0], o2_ref.shape[0]
    win = r1 + r2
    f1, f2 = acc_rows['a'][3], acc_rows['c'][3]
    e1, e2 = top_b, top_b + win
    last = [copy(norm_s.at[pl.ds(pl.multiple_of(f1 + (1 - core) * 8, 8), win), 0:half], pre_s.at[e1:e1 + win, 0:half],
                 send4.at[0], recv4.at[0], partner),
            copy(norm_s.at[f2:f2 + b2, 0:half], pre_s.at[e2:e2 + b2, 0:half], send4.at[1], recv4.at[1], partner)]
    own1 = norm_s[pl.ds(pl.multiple_of(f1 + core * 8, 8), win), 0:half]
    own2 = norm_s[f2:f2 + b2, 0:half]
    low = core == 0
    o1_ref[:, pl.ds(mine, half)] = jnp.where(low, own1[0:r1], own1[r2:win])
    o2_ref[:, pl.ds(mine, half)] = jnp.where(low, own2[0:r2], own2[r2:b2])
    for c in last:
        c.wait_recv()
    got1 = pre_s[e1:e1 + win, 0:half]
    got2 = pre_s[e2:e2 + b2, 0:half]
    o1_ref[:, pl.ds(his, half)] = jnp.where(low, got1[0:r1], got1[r2:win])
    o2_ref[:, pl.ds(his, half)] = jnp.where(low, got2[0:r2], got2[r2:b2])
    for c in started + last:
        c.wait_send()


def step_call(args, sizes):
    band, nm, edges, lat, feats = sizes
    steps = edges // CHUNK
    nt = band + band // 2
    dma = pltpu.SemaphoreType.DMA
    out_shape = (jax.ShapeDtypeStruct((nm, lat), BF), jax.ShapeDtypeStruct((band, lat), BF),
                 jax.ShapeDtypeStruct((feats, band), F32), jax.ShapeDtypeStruct((3 * lat // 128, lat), F32),
                 jax.ShapeDtypeStruct((lat // 128, lat), F32))
    return pl.pallas_call(
        step_kernel,
        out_shape=out_shape,
        in_specs=[pl.BlockSpec(memory_space=pl.ANY if k in FETCHED else VMEM) for k in range(len(args))],
        out_specs=(pl.BlockSpec(memory_space=VMEM),) * len(out_shape),
        scratch_shapes=[VMEM((edges, CHUNK), F32), VMEM((edges, CHUNK), F32), VMEM((steps * lat, CHUNK), BF),
                        VMEM((steps, 1, CHUNK), F32), VMEM((lat, 2 * lat + 3 * nm), BF), VMEM((lat, 3 * nm), BF),
                        VMEM((lat, nm), F32), VMEM((3 * lat, lat), F32), VMEM((lat, lat), F32), VMEM((lat, nt), BF),
                        VMEM((lat, nm), BF), VMEM((lat, lat), BF), VMEM((lat, lat), BF),
                        VMEM((128, lat), F32), VMEM((lat, 128), F32),
                        dma((7,)), pltpu.SemaphoreType.REGULAR, dma((2,)), dma((2,)), dma((2,)), dma((2,)),
                        dma((3,)), dma((3,)), dma((3, 3, 3)), dma((3, 3, 3)), dma((2,)), dma((2,))],
        compiler_params=pltpu.CompilerParams(collective_id=0, has_side_effects=True, vmem_limit_bytes=67043328),
        name='whole_step',
    )(*args)


def solution(mesh):
    row_spec = P(('batch', 'graph'), None)
    flat_spec = P(('batch', 'graph'))
    rep_spec = P(None, None)

    def device_step(grid_in, mesh_in, edge_in, edge_src, edge_dst, edge_mask, *rest):
        sizes = (grid_in.shape[0], mesh_in.shape[0], edge_in.shape[0], rest[1].shape[1], grid_in.shape[1])
        args = (grid_in.T, mesh_in.T, edge_in.T, edge_src[None], edge_dst[None], edge_mask[None]) + rest
        mesh_out, grid_out, ggrad, w1_grad, w2_grad = step_call(args, sizes)
        return mesh_out, grid_out, ggrad.T, w1_grad, w2_grad

    in_specs = (row_spec, row_spec, row_spec, flat_spec, flat_spec, flat_spec) + (rep_spec,) * 18 + (row_spec, row_spec)
    return jax.shard_map(device_step, mesh=mesh, in_specs=in_specs, out_specs=(row_spec,) * 5, check_vma=False)
```

```python
import jax
import jax.numpy as jnp
from jax import lax
from jax.experimental import pallas as pl
from jax.experimental.pallas import tpu as pltpu
from jax.sharding import PartitionSpec as P

NORM_EPS = 1e-5
BF = jnp.bfloat16
F32 = jnp.float32
VMEM = pltpu.VMEM
CHUNK = 512
FETCHED = (10, 13, 15, 18, 19, 21, 22, 25)
DEV = pl.DeviceIdType.MESH
GRID, MESH, EMBED, EDGE, NODE, POST = range(6)


def dot_nn(a, b):
    return jnp.dot(a, b, preferred_element_type=F32)


def dot_nt(a, b):
    return lax.dot_general(a, b, (((1,), (1,)), ((), ())), preferred_element_type=F32)


def dot_tn(a, b):
    return lax.dot_general(a, b, (((0,), (0,)), ((), ())), preferred_element_type=F32)


def split3(x):
    hi = x.astype(BF)
    rest = x - hi.astype(F32)
    mid = rest.astype(BF)
    low = (rest - mid.astype(F32)).astype(BF)
    return [hi, mid, low]


def silu_bf(p):
    h = 0.5 * p
    return (h + h * jnp.tanh(h)).astype(BF)


def norm_cols(q):
    centred = q - jnp.mean(q, axis=0, keepdims=True)
    inv = lax.rsqrt(jnp.mean(centred * centred, axis=0, keepdims=True) + NORM_EPS)
    return centred * inv, inv


def norm_back(d, n, inv):
    return inv * (d - jnp.mean(d, axis=0, keepdims=True) - n * jnp.mean(d * n, axis=0, keepdims=True))


def grad_first(d_act, p):
    t = jnp.tanh(0.5 * p)
    s = 0.5 + 0.5 * t
    return (d_act * (s * (1.0 + p * (1.0 - s)))).astype(BF)


def one_hot(rows, idx):
    return (lax.broadcasted_iota(jnp.int32, (rows, idx.shape[1]), 0) == idx).astype(F32).astype(BF)


def pick_lanes(ref, idx):
    outs = []
    for t in range(idx.shape[1] // 128):
        ix = idx[:, t * 128:(t + 1) * 128]
        low = jnp.broadcast_to(ix % 128, (ref.shape[0], 128))
        out = None
        for k in range(ref.shape[1] // 128):
            g = jnp.take_along_axis(ref[:, k * 128:(k + 1) * 128], low, axis=1, mode='promise_in_bounds')
            out = g if out is None else jnp.where(ix // 128 >= k, g, out)
        outs.append(out)
    return jnp.concatenate(outs, axis=1)


def lanes(*parts):
    return jnp.concatenate(parts, axis=1)


def rows(*parts):
    return jnp.concatenate(parts, axis=0)


def step_kernel(gx_ref, mx_ref, ex_ref, src_ref, dst_ref, mask_ref,
                gw1_ref, gw2_ref, gvec_ref, mw1_ref, mw2_ref, mvec_ref, ew1_ref, ew2_ref, evec_ref,
                dw1_ref, dw2_ref, dvec_ref, nw1_ref, nw2_ref, nvec_ref, pw1_ref, pw2_ref, pvec_ref,
                cotm_ref, cotg_ref,
                mesh_out_ref, grid_out_ref, ggrad_ref, o1_ref, o2_ref,
                pre_s, norm_s, he_s, inv_s, wl_s, pm_s, agg_s, g1_s, g2_s, act_s, cotg_s, w1g_s, w2g_s, table_s, hm_s, ew2t_s, dw2t_s, vt_s, vb_s, ew1t_s,
                stage_sem, done_sem, hs_sem, hr_sem, ts_sem, tr_sem, send0, recv0, sends, recvs, send4, recv4):
    lat = dw2_ref.shape[0]
    band = gx_ref.shape[1]
    nm = mx_ref.shape[1]
    halo = band // 4
    nt = band + 2 * halo
    ch = he_s.shape[1]
    steps = he_s.shape[0] // lat

    me = lax.axis_index('graph')
    total = 128
    core = lax.rem(me, 2)
    chip = me // 2
    px, py, pz = lax.rem(chip, 4), lax.rem(chip // 4, 4), chip // 16

    def dev(z, y, x, k):
        return {'graph': ((z * 4 + y) * 4 + x) * 2 + k}

    def turn(v, d):
        return lax.rem(v + d, 4)

    below = {'graph': lax.rem(me + total - 1, total)}
    above = {'graph': lax.rem(me + 1, total)}
    partner = dev(pz, py, px, 1 - core)
    peers = {'x': [dev(pz, py, turn(px, d), core) for d in (1, 2, 3)],
             'y': [dev(pz, turn(py, d), px, core) for d in (1, 2, 3)],
             'z': [dev(turn(pz, d), py, px, core) for d in (1, 2, 3)]}
    pos = {'x': px, 'y': py, 'z': pz}
    everyone = [below, above, partner] + peers['x'] + peers['y'] + peers['z']

    def fetch(k, src, slot):
        n = src.shape[0]
        return fetch_to(k, src, he_s.at[slot * lat:slot * lat + n, :])

    def fetch_to(k, src, dst):
        c = pltpu.make_async_copy(src, dst, stage_sem.at[k])
        c.start()
        return c

    def held(slot, n=1):
        return he_s[slot * lat:(slot + n) * lat, :]

    early = [fetch(0, mw2_ref, 15), fetch(1, dw1_ref, 10), fetch(2, ew2_ref, 14), fetch(4, pw1_ref, 5), fetch(5, pw2_ref, 6),
             fetch(6, cotg_ref, 7)]
    node = [fetch_to(7, nw1_ref.at[0:lat, :], g1_s), fetch_to(8, nw1_ref.at[lat:2 * lat, :], g2_s),
            fetch_to(9, nw2_ref, act_s)]

    barrier = pltpu.get_barrier_semaphore()
    for peer in everyone:
        pl.semaphore_signal(barrier, inc=1, device_id=peer, device_id_type=DEV)

    def copy(src, dst, ssem, rsem, peer):
        c = pltpu.make_async_remote_copy(src_ref=src, dst_ref=dst, send_sem=ssem, recv_sem=rsem, device_id=peer,
                                         device_id_type=DEV)
        c.start()
        return c

    v_s = pre_s.at[lat * steps - 128:lat * steps, :]
    v_s[...] = jnp.zeros(v_s.shape, F32)
    v_s[24:28, :] = ew1_ref[...].astype(F32)
    for k, ref in enumerate((gvec_ref, mvec_ref, evec_ref, dvec_ref, nvec_ref, pvec_ref)):
        v_s[4 * k:4 * k + 4, :] = ref[...]
    vt_s[...] = v_s[...].T
    ew1t_s[...] = vt_s[:, 24:28].astype(BF)

    def col(mlp, k):
        return vt_s[:, 4 * mlp + k:4 * mlp + k + 1]

    wide = [(EMBED, 0), (EMBED, 1), (EMBED, 2), (EMBED, 3), (EDGE, 1), (EDGE, 2), (EDGE, 3)]
    for j, (mlp, k) in enumerate(wide):
        vb_s[:, 128 * j:128 * (j + 1)] = jnp.broadcast_to(col(mlp, k), (lat, 128))

    def wcol(mlp, k):
        j = wide.index((mlp, k))
        v = vb_s[:, 128 * j:128 * (j + 1)]
        return lanes(*[v] * (ch // 128))

    def scaled(n, mlp, get=col):
        return n * get(mlp, 2) + get(mlp, 3)

    def grid_forward():
        p = dot_tn(gw1_ref[...], gx_ref[...].astype(BF)) + col(GRID, 0)
        n, inv = norm_cols(dot_tn(gw2_ref[...], silu_bf(p)) + col(GRID, 1))
        return p, n, inv

    table_s[:, halo:halo + band] = scaled(grid_forward()[1], GRID).astype(BF)
    for c in early:
        c.wait()
    mp = dot_tn(mw1_ref[...], mx_ref[...].astype(BF)) + col(MESH, 0)
    mn, _ = norm_cols(dot_tn(held(15), silu_bf(mp)) + col(MESH, 1))
    hm_s[...] = scaled(mn, MESH).astype(BF)

    pl.semaphore_wait(barrier, len(everyone))
    halos = [copy(table_s.at[:, halo:2 * halo], table_s.at[:, halo + band:nt], hs_sem.at[0], hr_sem.at[0], below),
             copy(table_s.at[:, band:band + halo], table_s.at[:, 0:halo], hs_sem.at[1], hr_sem.at[1], above)]

    hg = table_s[:, halo:halo + band]
    pp = dot_tn(held(5), hg) + col(POST, 0)
    pn, pinv = norm_cols(dot_tn(held(6), silu_bf(pp)) + col(POST, 1))
    grid_out_ref[...] = (hg.astype(F32) + scaled(pn, POST)).T.astype(BF)
    cg = held(7).astype(F32).T
    pd = norm_back(cg * col(POST, 2), pn, pinv)
    pg1 = grad_first(dot_nn(held(6), pd.astype(BF)), pp)
    cotg_s[...] = cg + dot_nn(held(5), pg1)

    wl_s[:, 0:lat] = held(10).T
    wl_s[:, lat:2 * lat] = held(11).T
    ew2t_s[...] = held(14).T
    dw2t_s[...] = dw2_ref[...].T
    pm_s[...] = dot_tn(held(12), hm_s[...]) + col(EDGE, 0)
    agg_s[...] = jnp.zeros_like(agg_s)
    base = me * band - halo

    def slab(i):
        return pl.ds(pl.multiple_of(i * ch, ch), ch)

    def masked_dst(sl):
        return jnp.where(mask_ref[:, sl] > 0, dst_ref[:, sl], -1)

    def embed(i):
        pe = dot_nn(ew1t_s[...], ex_ref[:, slab(i)].astype(BF)) + wcol(EMBED, 0)
        ne, _ = norm_cols(dot_nn(ew2t_s[...], silu_bf(pe)) + wcol(EMBED, 1))
        he_s[slab(i), :] = scaled(ne, EMBED, wcol).astype(BF)

    def first_half(i):
        sl = slab(i)
        gath = dot_nn(table_s[...], one_hot(nt, src_ref[:, sl] - base)).astype(BF)
        pre_s[sl, :] = dot_nn(wl_s[...], rows(he_s[sl, :], gath)) + pick_lanes(pm_s, dst_ref[:, sl])

    def second_half(i):
        sl = slab(i)
        n, inv = norm_cols(dot_nn(dw2t_s[...], silu_bf(pre_s[sl, :])) + wcol(EDGE, 1))
        norm_s[sl, :] = n
        inv_s[i] = inv
        msg = he_s[sl, :].astype(F32) + scaled(n, EDGE, wcol)
        ohm = one_hot(nm, masked_dst(sl))
        agg_s[...] += dot_nt(lanes(*split3(msg)), lanes(ohm, ohm, ohm))

    def fwd(i, carry):
        second_half(i - 1)
        first_half(i)
        embed(jnp.minimum(i + 1, steps - 1))
        return carry

    embed(0)
    embed(1)
    for c in halos:
        c.wait_recv()
    first_half(0)
    lax.fori_loop(1, steps, fwd, 0)
    second_half(steps - 1)

    for c in node:
        c.wait()
    hm = hm_s[...]
    np_ = dot_tn(rows(g1_s[...], g2_s[...]), rows(hm, agg_s[...].astype(BF))) + col(NODE, 0)
    nn_, ninv = norm_cols(dot_tn(act_s[...], silu_bf(np_)) + col(NODE, 1))
    mesh_out_ref[...] = (hm.astype(F32) + scaled(nn_, NODE)).T.astype(BF)
    d2 = norm_back(cotm_ref[...].astype(F32).T * col(NODE, 2), nn_, ninv)
    ng1 = grad_first(dot_nn(act_s[...], d2.astype(BF)), np_)
    ag = dot_nn(g2_s[...], ng1) * col(EDGE, 2)
    pm_s[...] = ag - jnp.mean(ag, axis=0, keepdims=True)

    w1g_s[...] = jnp.zeros_like(w1g_s)
    w2g_s[...] = jnp.zeros_like(w2g_s)

    slots = [(g1_s.at[:, :], g2_s.at[:, :], act_s.at[:, :]),
             (wl_s.at[:, 0:lat], wl_s.at[:, lat:2 * lat], ew2t_s.at[:, :])]

    def second_grad(i, slot):
        sl = slab(i)
        bg = jnp.where(mask_ref[:, sl] > 0, pick_lanes(pm_s, dst_ref[:, sl]), 0.0)
        n = norm_s[sl, :]
        slots[slot][1][...] = (inv_s[i] * (bg - n * jnp.mean(bg * n, axis=0, keepdims=True))).astype(BF)

    def first_grad(i, slot):
        p = pre_s[slab(i), :]
        d_act = dot_nn(dw2_ref[...], slots[slot][1][...])
        slots[slot][2][...] = silu_bf(p)
        slots[slot][0][...] = grad_first(d_act, p)

    def sums(i, slot):
        sl = slab(i)
        g1, g2, act = slots[slot]
        w2g_s[...] += dot_nt(act[...], g2[...])
        w1g_s[...] += dot_nt(rows(he_s[sl, :], one_hot(nt, src_ref[:, sl] - base), one_hot(nm, masked_dst(sl))), g1[...])

    def bwd(j, carry):
        i = 2 * j
        first_grad(i - 1, 1)
        sums(i - 2, 0)
        second_grad(i, 0)
        first_grad(i, 0)
        sums(i - 1, 1)
        second_grad(i + 1, 1)
        return carry

    second_grad(0, 0)
    first_grad(0, 0)
    second_grad(1, 1)
    lax.fori_loop(1, steps // 2, bwd, 0)
    for peer in everyone:
        pl.semaphore_signal(done_sem, inc=1, device_id=peer, device_id_type=DEV)
    first_grad(steps - 1, 1)
    sums(steps - 2, 0)
    sums(steps - 1, 1)

    half = lat // 2
    q = half // 2
    mine = pl.multiple_of(core * half, half)
    his = pl.multiple_of((1 - core) * half, half)
    his_b = pl.multiple_of(his + q, q)
    n1, n2 = 3 * lat, lat

    def swap(k, src, top, c0, w, j):
        return copy(src, pre_s.at[top:top + src.shape[0], c0:c0 + w], send0.at[j], recv0.at[j], partner)

    pl.semaphore_wait(done_sem, len(everyone))
    late = [fetch(3, dw1_ref.at[lat:2 * lat, :], 8)]
    first = {'c': [swap('c', w2g_s.at[:, pl.ds(his, half)], n1, 0, half, 0)],
             'a': [swap('a', w1g_s.at[0:lat, pl.ds(his, q)], 0, 0, q, 1)],
             'b': [swap('b', w1g_s.at[0:lat, pl.ds(his_b, q)], 0, q, q, 2)]}
    for k, part in enumerate(split3(w1g_s[lat:lat + nt, :])):
        he_s[k * nt:(k + 1) * nt, :] = part
    t0 = 9 * lat
    for k, part in enumerate(split3(w1g_s[lat + nt:lat + nt + nm, :])):
        he_s[t0 + k * nm:t0 + (k + 1) * nm, :] = part
    tb = table_s[...]
    w1g_s[lat:2 * lat, :] = dot_nn(lanes(tb, tb, tb), he_s[0:3 * nt, :])
    w1g_s[2 * lat:3 * lat, :] = dot_nn(lanes(hm, hm, hm), he_s[t0:t0 + 3 * nm, :])
    first['a'].append(swap('a', w1g_s.at[lat:n1, pl.ds(his, q)], lat, 0, q, 3))
    first['b'].append(swap('b', w1g_s.at[lat:n1, pl.ds(his_b, q)], lat, q, q, 4))

    b1, b2 = n1 // 64, n2 // 64
    shape = {'a': (b1, 0, q), 'b': (b1, q, q), 'c': (b2, 0, half)}
    axes = {'a': 'xyz', 'b': 'yzx', 'c': 'zxy'}
    order = 'cab'
    at = {'a': 0, 'b': 0, 'c': n1}
    acc_rows = {k: [] for k in order}
    buf_rows = {k: [] for k in order}
    top_a, top_b = 4 * lat, n1 + n2
    for stage in range(4):
        for k in 'ac':
            acc_rows[k].append(top_a)
            top_a += shape[k][0] * 4 ** (3 - stage)
            buf_rows[k].append(top_b)
            top_b += 0 if stage == 3 else 3 * shape[k][0] * 4 ** (2 - stage)
    acc_rows['b'], buf_rows['b'] = acc_rows['a'], buf_rows['a']

    def acc_at(k, stage, off, n):
        return norm_s.at[pl.ds(acc_rows[k][stage] + off, n), shape[k][1]:shape[k][1] + shape[k][2]]

    def buf_at(k, stage, off, n):
        return pre_s.at[pl.ds(buf_rows[k][stage] + off, n), shape[k][1]:shape[k][1] + shape[k][2]]

    def send(k, stage, j, src_off, dst_off, n, d):
        c = copy(acc_at(k, stage, src_off, n), buf_at(k, stage, dst_off, n), sends.at[order.index(k), stage, j],
                 recvs.at[order.index(k), stage, j], peers[axes[k][stage]][d - 1])
        started.append(c)
        return c

    def block(k, stage, d, n, off=0):
        return pl.multiple_of(turn(pos[axes[k][stage]], d) * n + off, 8)

    def launch(k, stage):
        n = shape[k][0] * 4 ** (2 - stage)
        return [send(k, stage, d - 1, block(k, stage, d, n), (d - 1) * n, n, d) for d in (2, 1, 3)]

    started = list(halos)
    flying = {}

    def open_first(k):
        n, c0, w = shape[k]
        for c in first[k]:
            c.wait_recv()
            started.append(c)
        src = w2g_s if k == 'c' else w1g_s
        for i in range(64):
            v = {'z': i // 16, 'y': i // 4 % 4, 'x': i % 4}
            to = (v[axes[k][0]] * 4 + v[axes[k][1]]) * 4 + v[axes[k][2]]
            acc_at(k, 0, to * n, n)[...] = (src[i * n:(i + 1) * n, pl.ds(pl.multiple_of(mine + c0, q), w)]
                                            + pre_s[at[k] + i * n:at[k] + (i + 1) * n, c0:c0 + w])
        n = n * 16
        h = n // 2
        flying[k] = [send(k, 0, 0, block(k, 0, 2, n), 0, h, 1), send(k, 0, 1, block(k, 0, 2, n, h), h, h, 3),
                     send(k, 0, 2, block(k, 0, 1, n, h), n + h, h, 1), send(k, 0, 3, block(k, 0, 3, n), 2 * n, h, 3)]

    def relay_first(k):
        n = shape[k][0] * 16
        h = n // 2
        for j, d, off, dst in ((0, 1, 0, n), (1, 3, h, 2 * n + h)):
            flying[k][j].wait_recv()
            to = acc_at(k, 0, block(k, 0, d, n, off), h)
            to[...] = to[...] + buf_at(k, 0, j * h, h)[...]
            flying[k].append(send(k, 0, 4 + j, block(k, 0, d, n, off), dst, h, d))

    def close_first(k):
        n = shape[k][0] * 16
        for c in flying[k][2:]:
            c.wait_recv()
        acc_at(k, 1, 0, n)[...] = acc_at(k, 0, block(k, 0, 0, n), n)[...] + (
            buf_at(k, 0, n, n)[...] + buf_at(k, 0, 2 * n, n)[...])
        flying[k] = launch(k, 1)

    open_first('c')
    for c in late:
        c.wait()
    wb = held(8)
    tg = dot_nt(lanes(wb, wb, wb), lanes(he_s[0:nt, :], he_s[nt:2 * nt, :], he_s[2 * nt:3 * nt, :]))
    norm_s[0:lat, 0:halo] = tg[:, 0:halo]
    norm_s[0:lat, halo:2 * halo] = tg[:, halo + band:nt]
    norm_s[lat:2 * lat, :] = tg[:, halo:halo + band]
    tails = [copy(norm_s.at[0:lat, 0:halo], pre_s.at[0:lat, 2 * halo:3 * halo], ts_sem.at[0], tr_sem.at[0], below),
             copy(norm_s.at[0:lat, halo:2 * halo], pre_s.at[0:lat, 3 * halo:4 * halo], ts_sem.at[1], tr_sem.at[1],
                  above)]
    started += tails
    open_first('a')
    open_first('b')

    gp, gn, ginv = grid_forward()
    keep_p, keep_n = slice(10 * lat, 11 * lat), slice(11 * lat, 12 * lat)
    norm_s[keep_p, :] = gp
    norm_s[keep_n, :] = gn
    inv_s[0] = ginv
    relay_first('c')
    relay_first('a')
    relay_first('b')
    own = cotg_s[...] + norm_s[lat:2 * lat, :]

    for c in tails:
        c.wait_recv()
    ends = lanes(own[:, 0:halo] + pre_s[0:lat, 3 * halo:4 * halo], own[:, halo:band - halo],
                 own[:, band - halo:band] + pre_s[0:lat, 2 * halo:3 * halo])
    gd = norm_back(ends * col(GRID, 2), norm_s[keep_n, :], inv_s[0])
    close_first('c')
    gg1 = grad_first(dot_nn(gw2_ref[...], gd.astype(BF)), norm_s[keep_p, :])
    ggrad_ref[...] = dot_nn(gw1_ref[...], gg1)
    close_first('a')
    close_first('b')

    for stage in (1, 2):
        for k in order:
            for c in flying[k]:
                c.wait_recv()
            n = shape[k][0] * 4 ** (2 - stage)
            acc_at(k, stage + 1, 0, n)[...] = (
                acc_at(k, stage, block(k, stage, 0, n), n)[...] + buf_at(k, stage, 0, n)[...]) + (
                buf_at(k, stage, n, n)[...] + buf_at(k, stage, 2 * n, n)[...])
            if stage < 2:
                flying[k] = launch(k, stage + 1)

    r1, r2 = o1_ref.shape[0], o2_ref.shape[0]
    win = r1 + r2
    f1, f2 = acc_rows['a'][3], acc_rows['c'][3]
    e1, e2 = top_b, top_b + win
    last = [copy(norm_s.at[pl.ds(pl.multiple_of(f1 + (1 - core) * 8, 8), win), 0:half], pre_s.at[e1:e1 + win, 0:half],
                 send4.at[0], recv4.at[0], partner),
            copy(norm_s.at[f2:f2 + b2, 0:half], pre_s.at[e2:e2 + b2, 0:half], send4.at[1], recv4.at[1], partner)]
    own1 = norm_s[pl.ds(pl.multiple_of(f1 + core * 8, 8), win), 0:half]
    own2 = norm_s[f2:f2 + b2, 0:half]
    low = core == 0
    o1_ref[:, pl.ds(mine, half)] = jnp.where(low, own1[0:r1], own1[r2:win])
    o2_ref[:, pl.ds(mine, half)] = jnp.where(low, own2[0:r2], own2[r2:b2])
    for c in last:
        c.wait_recv()
    got1 = pre_s[e1:e1 + win, 0:half]
    got2 = pre_s[e2:e2 + b2, 0:half]
    o1_ref[:, pl.ds(his, half)] = jnp.where(low, got1[0:r1], got1[r2:win])
    o2_ref[:, pl.ds(his, half)] = jnp.where(low, got2[0:r2], got2[r2:b2])
    for c in started + last:
        c.wait_send()


def finish_kernel(*refs):
    n = (len(refs) - 1) // 3
    bufs, sems = refs[2 * n:3 * n], refs[3 * n]
    ins = [pltpu.make_async_copy(refs[k], bufs[k], sems.at[0, k]) for k in range(n)]
    outs = [pltpu.make_async_copy(bufs[k], refs[n + k], sems.at[1, k]) for k in range(n)]
    for c in ins:
        c.start()
    for c, o in zip(ins, outs):
        c.wait()
        o.start()
    for o in outs:
        o.wait()


def finish_call(outs):
    n = len(outs)
    return pl.pallas_call(
        finish_kernel,
        out_shape=tuple(jax.ShapeDtypeStruct(o.shape, o.dtype) for o in outs),
        in_specs=[pl.BlockSpec(memory_space=pl.ANY)] * n,
        out_specs=(pl.BlockSpec(memory_space=pl.ANY),) * n,
        scratch_shapes=[VMEM(o.shape, o.dtype) for o in outs] + [pltpu.SemaphoreType.DMA((2, n))],
        compiler_params=pltpu.CompilerParams(vmem_limit_bytes=67043328),
        name='finish',
    )(*outs)


def step_call(args, sizes):
    band, nm, edges, lat, feats = sizes
    steps = edges // CHUNK
    nt = band + band // 2
    dma = pltpu.SemaphoreType.DMA
    out_shape = (jax.ShapeDtypeStruct((nm, lat), BF), jax.ShapeDtypeStruct((band, lat), BF),
                 jax.ShapeDtypeStruct((feats, band), F32), jax.ShapeDtypeStruct((3 * lat // 128, lat), F32),
                 jax.ShapeDtypeStruct((lat // 128, lat), F32))
    return pl.pallas_call(
        step_kernel,
        out_shape=out_shape,
        in_specs=[pl.BlockSpec(memory_space=pl.ANY if k in FETCHED else VMEM) for k in range(len(args))],
        out_specs=(pl.BlockSpec(memory_space=VMEM),) * len(out_shape),
        scratch_shapes=[VMEM((edges, CHUNK), F32), VMEM((edges, CHUNK), F32), VMEM((steps * lat, CHUNK), BF),
                        VMEM((steps, 1, CHUNK), F32), VMEM((lat, 2 * lat), BF), VMEM((lat, nm), F32),
                        VMEM((lat, nm), F32), VMEM((lat, CHUNK), BF), VMEM((lat, CHUNK), BF), VMEM((lat, CHUNK), BF),
                        VMEM((lat, band), F32),
                        VMEM((3 * lat, lat), F32), VMEM((lat, lat), F32), VMEM((lat, nt), BF),
                        VMEM((lat, nm), BF), VMEM((lat, lat), BF), VMEM((lat, lat), BF),
                        VMEM((lat, 128), F32), VMEM((lat, 7 * 128), F32), VMEM((lat, 4), BF),
                        dma((10,)), pltpu.SemaphoreType.REGULAR, dma((2,)), dma((2,)), dma((2,)), dma((2,)),
                        dma((5,)), dma((5,)), dma((3, 3, 6)), dma((3, 3, 6)), dma((2,)), dma((2,))],
        compiler_params=pltpu.CompilerParams(collective_id=0, has_side_effects=True, vmem_limit_bytes=67043328),
        name='whole_step',
    )(*args)


def solution(mesh):
    row_spec = P(('batch', 'graph'), None)
    flat_spec = P(('batch', 'graph'))
    rep_spec = P(None, None)

    def device_step(grid_in, mesh_in, edge_in, edge_src, edge_dst, edge_mask, *rest):
        sizes = (grid_in.shape[0], mesh_in.shape[0], edge_in.shape[0], rest[1].shape[1], grid_in.shape[1])
        args = (grid_in.T, mesh_in.T, edge_in.T, edge_src[None], edge_dst[None], edge_mask[None]) + rest
        mesh_out, grid_out, ggrad, w1_grad, w2_grad = finish_call(step_call(args, sizes))
        return mesh_out, grid_out, ggrad.T, w1_grad, w2_grad

    in_specs = (row_spec, row_spec, row_spec, flat_spec, flat_spec, flat_spec) + (rep_spec,) * 18 + (row_spec, row_spec)
    return jax.shard_map(device_step, mesh=mesh, in_specs=in_specs, out_specs=(row_spec,) * 5, check_vma=False)
```

```python
import jax
import jax.numpy as jnp
from jax import lax
from jax.experimental import pallas as pl
from jax.experimental.pallas import tpu as pltpu
from jax.sharding import PartitionSpec as P

NORM_EPS = 1e-5
BF = jnp.bfloat16
F32 = jnp.float32
VMEM = pltpu.VMEM
CHUNK = 512
FETCHED = (10, 13, 15, 18, 19, 21, 22, 25)
DEV = pl.DeviceIdType.MESH
GRID, MESH, EMBED, EDGE, NODE, POST = range(6)


def dot_nn(a, b):
    return jnp.dot(a, b, preferred_element_type=F32)


def dot_nt(a, b):
    return lax.dot_general(a, b, (((1,), (1,)), ((), ())), preferred_element_type=F32)


def dot_tn(a, b):
    return lax.dot_general(a, b, (((0,), (0,)), ((), ())), preferred_element_type=F32)


def split3(x):
    hi = x.astype(BF)
    rest = x - hi.astype(F32)
    mid = rest.astype(BF)
    low = (rest - mid.astype(F32)).astype(BF)
    return [hi, mid, low]


def silu_bf(p):
    h = 0.5 * p
    return (h + h * jnp.tanh(h)).astype(BF)


def norm_cols(q):
    centred = q - jnp.mean(q, axis=0, keepdims=True)
    inv = lax.rsqrt(jnp.mean(centred * centred, axis=0, keepdims=True) + NORM_EPS)
    return centred * inv, inv


def norm_back(d, n, inv):
    return inv * (d - jnp.mean(d, axis=0, keepdims=True) - n * jnp.mean(d * n, axis=0, keepdims=True))


def grad_first(d_act, p):
    t = jnp.tanh(0.5 * p)
    s = 0.5 + 0.5 * t
    return (d_act * (s * (1.0 + p * (1.0 - s)))).astype(BF)


def one_hot(rows, idx):
    return (lax.broadcasted_iota(jnp.int32, (rows, idx.shape[1]), 0) == idx).astype(F32).astype(BF)


def pick_lanes(ref, idx):
    outs = []
    for t in range(idx.shape[1] // 128):
        ix = idx[:, t * 128:(t + 1) * 128]
        low = jnp.broadcast_to(ix % 128, (ref.shape[0], 128))
        out = None
        for k in range(ref.shape[1] // 128):
            g = jnp.take_along_axis(ref[:, k * 128:(k + 1) * 128], low, axis=1, mode='promise_in_bounds')
            out = g if out is None else jnp.where(ix // 128 >= k, g, out)
        outs.append(out)
    return jnp.concatenate(outs, axis=1)


def lanes(*parts):
    return jnp.concatenate(parts, axis=1)


def rows(*parts):
    return jnp.concatenate(parts, axis=0)


def step_kernel(gx_ref, mx_ref, ex_ref, src_ref, dst_ref, mask_ref,
                gw1_ref, gw2_ref, gvec_ref, mw1_ref, mw2_ref, mvec_ref, ew1_ref, ew2_ref, evec_ref,
                dw1_ref, dw2_ref, dvec_ref, nw1_ref, nw2_ref, nvec_ref, pw1_ref, pw2_ref, pvec_ref,
                cotm_ref, cotg_ref,
                mesh_out_ref, grid_out_ref, ggrad_ref, o1_ref, o2_ref,
                pre_s, norm_s, he_s, inv_s, wl_s, pm_s, agg_s, g1_s, g2_s, act_s, cotg_s, w1g_s, w2g_s, table_s, hm_s, ew2t_s, dw2t_s, vt_s, vb_s, ew1t_s,
                stage_sem, done_sem, hs_sem, hr_sem, ts_sem, tr_sem, send0, recv0, sends, recvs, send4, recv4):
    lat = dw2_ref.shape[0]
    band = gx_ref.shape[1]
    nm = mx_ref.shape[1]
    halo = band // 4
    nt = band + 2 * halo
    ch = he_s.shape[1]
    steps = he_s.shape[0] // lat

    me = lax.axis_index('graph')
    total = 128
    core = lax.rem(me, 2)
    chip = me // 2
    px, py, pz = lax.rem(chip, 4), lax.rem(chip // 4, 4), chip // 16

    def dev(z, y, x, k):
        return {'graph': ((z * 4 + y) * 4 + x) * 2 + k}

    def turn(v, d):
        return lax.rem(v + d, 4)

    below = {'graph': lax.rem(me + total - 1, total)}
    above = {'graph': lax.rem(me + 1, total)}
    partner = dev(pz, py, px, 1 - core)
    peers = {'x': [dev(pz, py, turn(px, d), core) for d in (1, 2, 3)],
             'y': [dev(pz, turn(py, d), px, core) for d in (1, 2, 3)],
             'z': [dev(turn(pz, d), py, px, core) for d in (1, 2, 3)]}
    pos = {'x': px, 'y': py, 'z': pz}
    everyone = [below, above, partner] + peers['x'] + peers['y'] + peers['z']

    def fetch(k, src, slot):
        n = src.shape[0]
        return fetch_to(k, src, he_s.at[slot * lat:slot * lat + n, :])

    def fetch_to(k, src, dst):
        c = pltpu.make_async_copy(src, dst, stage_sem.at[k])
        c.start()
        return c

    def held(slot, n=1):
        return he_s[slot * lat:(slot + n) * lat, :]

    early = [fetch(0, mw2_ref, 15), fetch(1, dw1_ref, 10), fetch(2, ew2_ref, 14), fetch(4, pw1_ref, 5), fetch(5, pw2_ref, 6),
             fetch(6, cotg_ref, 7)]
    node = [fetch_to(7, nw1_ref.at[0:lat, :], g1_s), fetch_to(8, nw1_ref.at[lat:2 * lat, :], g2_s),
            fetch_to(9, nw2_ref, act_s)]

    barrier = pltpu.get_barrier_semaphore()
    for peer in everyone:
        pl.semaphore_signal(barrier, inc=1, device_id=peer, device_id_type=DEV)

    def copy(src, dst, ssem, rsem, peer):
        c = pltpu.make_async_remote_copy(src_ref=src, dst_ref=dst, send_sem=ssem, recv_sem=rsem, device_id=peer,
                                         device_id_type=DEV)
        c.start()
        return c

    v_s = pre_s.at[lat * steps - 128:lat * steps, :]
    v_s[...] = jnp.zeros(v_s.shape, F32)
    v_s[24:28, :] = ew1_ref[...].astype(F32)
    for k, ref in enumerate((gvec_ref, mvec_ref, evec_ref, dvec_ref, nvec_ref, pvec_ref)):
        v_s[4 * k:4 * k + 4, :] = ref[...]
    vt_s[...] = v_s[...].T
    ew1t_s[...] = vt_s[:, 24:28].astype(BF)

    def col(mlp, k):
        return vt_s[:, 4 * mlp + k:4 * mlp + k + 1]

    wide = [(EMBED, 0), (EMBED, 1), (EMBED, 2), (EMBED, 3), (EDGE, 1), (EDGE, 2), (EDGE, 3)]
    for j, (mlp, k) in enumerate(wide):
        vb_s[:, 128 * j:128 * (j + 1)] = jnp.broadcast_to(col(mlp, k), (lat, 128))

    def wcol(mlp, k):
        j = wide.index((mlp, k))
        v = vb_s[:, 128 * j:128 * (j + 1)]
        return lanes(*[v] * (ch // 128))

    def scaled(n, mlp, get=col):
        return n * get(mlp, 2) + get(mlp, 3)

    def grid_forward():
        p = dot_tn(gw1_ref[...], gx_ref[...].astype(BF)) + col(GRID, 0)
        n, inv = norm_cols(dot_tn(gw2_ref[...], silu_bf(p)) + col(GRID, 1))
        return p, n, inv

    table_s[:, halo:halo + band] = scaled(grid_forward()[1], GRID).astype(BF)
    for c in early:
        c.wait()
    mp = dot_tn(mw1_ref[...], mx_ref[...].astype(BF)) + col(MESH, 0)
    mn, _ = norm_cols(dot_tn(held(15), silu_bf(mp)) + col(MESH, 1))
    hm_s[...] = scaled(mn, MESH).astype(BF)

    pl.semaphore_wait(barrier, len(everyone))
    halos = [copy(table_s.at[:, halo:2 * halo], table_s.at[:, halo + band:nt], hs_sem.at[0], hr_sem.at[0], below),
             copy(table_s.at[:, band:band + halo], table_s.at[:, 0:halo], hs_sem.at[1], hr_sem.at[1], above)]

    hg = table_s[:, halo:halo + band]
    pp = dot_tn(held(5), hg) + col(POST, 0)
    pn, pinv = norm_cols(dot_tn(held(6), silu_bf(pp)) + col(POST, 1))
    grid_out_ref[...] = (hg.astype(F32) + scaled(pn, POST)).T.astype(BF)
    cg = held(7).astype(F32).T
    pd = norm_back(cg * col(POST, 2), pn, pinv)
    pg1 = grad_first(dot_nn(held(6), pd.astype(BF)), pp)
    cotg_s[...] = cg + dot_nn(held(5), pg1)

    wl_s[:, 0:lat] = held(10).T
    wl_s[:, lat:2 * lat] = held(11).T
    ew2t_s[...] = held(14).T
    dw2t_s[...] = dw2_ref[...].T
    pm_s[...] = dot_tn(held(12), hm_s[...]) + col(EDGE, 0)
    agg_s[...] = jnp.zeros_like(agg_s)
    base = me * band - halo

    def slab(i):
        return pl.ds(pl.multiple_of(i * ch, ch), ch)

    def masked_dst(sl):
        return jnp.where(mask_ref[:, sl] > 0, dst_ref[:, sl], -1)

    def embed(i):
        pe = dot_nn(ew1t_s[...], ex_ref[:, slab(i)].astype(BF)) + wcol(EMBED, 0)
        ne, _ = norm_cols(dot_nn(ew2t_s[...], silu_bf(pe)) + wcol(EMBED, 1))
        he_s[slab(i), :] = scaled(ne, EMBED, wcol).astype(BF)

    def first_half(i):
        sl = slab(i)
        gath = dot_nn(table_s[...], one_hot(nt, src_ref[:, sl] - base)).astype(BF)
        pre_s[sl, :] = dot_nn(wl_s[...], rows(he_s[sl, :], gath)) + pick_lanes(pm_s, dst_ref[:, sl])

    def second_half(i):
        sl = slab(i)
        n, inv = norm_cols(dot_nn(dw2t_s[...], silu_bf(pre_s[sl, :])) + wcol(EDGE, 1))
        norm_s[sl, :] = n
        inv_s[i] = inv
        msg = he_s[sl, :].astype(F32) + scaled(n, EDGE, wcol)
        ohm = one_hot(nm, masked_dst(sl))
        agg_s[...] += dot_nt(lanes(*split3(msg)), lanes(ohm, ohm, ohm))

    def fwd(i, carry):
        second_half(i - 1)
        embed(jnp.minimum(i + 1, steps - 1))
        first_half(i)
        return carry

    embed(0)
    embed(1)
    for c in halos:
        c.wait_recv()
    first_half(0)
    lax.fori_loop(1, steps, fwd, 0)
    second_half(steps - 1)

    for c in node:
        c.wait()
    hm = hm_s[...]
    np_ = dot_tn(rows(g1_s[...], g2_s[...]), rows(hm, agg_s[...].astype(BF))) + col(NODE, 0)
    nn_, ninv = norm_cols(dot_tn(act_s[...], silu_bf(np_)) + col(NODE, 1))
    mesh_out_ref[...] = (hm.astype(F32) + scaled(nn_, NODE)).T.astype(BF)
    d2 = norm_back(cotm_ref[...].astype(F32).T * col(NODE, 2), nn_, ninv)
    ng1 = grad_first(dot_nn(act_s[...], d2.astype(BF)), np_)
    ag = dot_nn(g2_s[...], ng1) * col(EDGE, 2)
    pm_s[...] = ag - jnp.mean(ag, axis=0, keepdims=True)

    w1g_s[...] = jnp.zeros_like(w1g_s)
    w2g_s[...] = jnp.zeros_like(w2g_s)

    slots = [(g1_s.at[:, :], g2_s.at[:, :], act_s.at[:, :]),
             (wl_s.at[:, 0:lat], wl_s.at[:, lat:2 * lat], ew2t_s.at[:, :])]

    def second_grad(i, slot):
        sl = slab(i)
        bg = jnp.where(mask_ref[:, sl] > 0, pick_lanes(pm_s, dst_ref[:, sl]), 0.0)
        n = norm_s[sl, :]
        slots[slot][1][...] = (inv_s[i] * (bg - n * jnp.mean(bg * n, axis=0, keepdims=True))).astype(BF)

    def first_grad(i, slot):
        p = pre_s[slab(i), :]
        d_act = dot_nn(dw2_ref[...], slots[slot][1][...])
        slots[slot][2][...] = silu_bf(p)
        slots[slot][0][...] = grad_first(d_act, p)

    def sums(i, slot):
        sl = slab(i)
        g1, g2, act = slots[slot]
        w2g_s[...] += dot_nt(act[...], g2[...])
        w1g_s[...] += dot_nt(rows(he_s[sl, :], one_hot(nt, src_ref[:, sl] - base), one_hot(nm, masked_dst(sl))), g1[...])

    def bwd(j, carry):
        i = 2 * j
        first_grad(i - 1, 1)
        sums(i - 2, 0)
        second_grad(i, 0)
        first_grad(i, 0)
        sums(i - 1, 1)
        second_grad(i + 1, 1)
        return carry

    second_grad(0, 0)
    first_grad(0, 0)
    second_grad(1, 1)
    lax.fori_loop(1, steps // 2, bwd, 0)
    for peer in everyone:
        pl.semaphore_signal(done_sem, inc=1, device_id=peer, device_id_type=DEV)
    first_grad(steps - 1, 1)
    sums(steps - 2, 0)
    sums(steps - 1, 1)

    half = lat // 2
    q = half // 2
    mine = pl.multiple_of(core * half, half)
    his = pl.multiple_of((1 - core) * half, half)
    his_b = pl.multiple_of(his + q, q)
    n1, n2 = 3 * lat, lat

    def swap(k, src, top, c0, w, j):
        return copy(src, pre_s.at[top:top + src.shape[0], c0:c0 + w], send0.at[j], recv0.at[j], partner)

    pl.semaphore_wait(done_sem, len(everyone))
    late = [fetch(3, dw1_ref.at[lat:2 * lat, :], 8)]
    first = {'c': [swap('c', w2g_s.at[:, pl.ds(his, half)], n1, 0, half, 0)],
             'a': [swap('a', w1g_s.at[0:lat, pl.ds(his, q)], 0, 0, q, 1)],
             'b': [swap('b', w1g_s.at[0:lat, pl.ds(his_b, q)], 0, q, q, 2)]}
    for k, part in enumerate(split3(w1g_s[lat:lat + nt, :])):
        he_s[k * nt:(k + 1) * nt, :] = part
    t0 = 9 * lat
    for k, part in enumerate(split3(w1g_s[lat + nt:lat + nt + nm, :])):
        he_s[t0 + k * nm:t0 + (k + 1) * nm, :] = part
    tb = table_s[...]
    w1g_s[lat:2 * lat, :] = dot_nn(lanes(tb, tb, tb), he_s[0:3 * nt, :])
    w1g_s[2 * lat:3 * lat, :] = dot_nn(lanes(hm, hm, hm), he_s[t0:t0 + 3 * nm, :])
    first['a'].append(swap('a', w1g_s.at[lat:n1, pl.ds(his, q)], lat, 0, q, 3))
    first['b'].append(swap('b', w1g_s.at[lat:n1, pl.ds(his_b, q)], lat, q, q, 4))

    b1, b2 = n1 // 64, n2 // 64
    shape = {'a': (b1, 0, q), 'b': (b1, q, q), 'c': (b2, 0, half)}
    axes = {'a': 'xyz', 'b': 'yzx', 'c': 'zxy'}
    order = 'cab'
    at = {'a': 0, 'b': 0, 'c': n1}
    acc_rows = {k: [] for k in order}
    buf_rows = {k: [] for k in order}
    top_a, top_b = 4 * lat, n1 + n2
    for stage in range(4):
        for k in 'ac':
            acc_rows[k].append(top_a)
            top_a += shape[k][0] * 4 ** (3 - stage)
            buf_rows[k].append(top_b)
            top_b += 0 if stage == 3 else 3 * shape[k][0] * 4 ** (2 - stage)
    acc_rows['b'], buf_rows['b'] = acc_rows['a'], buf_rows['a']

    def acc_at(k, stage, off, n):
        return norm_s.at[pl.ds(acc_rows[k][stage] + off, n), shape[k][1]:shape[k][1] + shape[k][2]]

    def buf_at(k, stage, off, n):
        return pre_s.at[pl.ds(buf_rows[k][stage] + off, n), shape[k][1]:shape[k][1] + shape[k][2]]

    def send(k, stage, j, src_off, dst_off, n, d):
        c = copy(acc_at(k, stage, src_off, n), buf_at(k, stage, dst_off, n), sends.at[order.index(k), stage, j],
                 recvs.at[order.index(k), stage, j], peers[axes[k][stage]][d - 1])
        started.append(c)
        return c

    def block(k, stage, d, n, off=0):
        return pl.multiple_of(turn(pos[axes[k][stage]], d) * n + off, 8)

    def launch(k, stage):
        n = shape[k][0] * 4 ** (2 - stage)
        return [send(k, stage, d - 1, block(k, stage, d, n), (d - 1) * n, n, d) for d in (2, 1, 3)]

    started = list(halos)
    flying = {}

    def open_first(k):
        n, c0, w = shape[k]
        for c in first[k]:
            c.wait_recv()
            started.append(c)
        src = w2g_s if k == 'c' else w1g_s
        for i in range(64):
            v = {'z': i // 16, 'y': i // 4 % 4, 'x': i % 4}
            to = (v[axes[k][0]] * 4 + v[axes[k][1]]) * 4 + v[axes[k][2]]
            acc_at(k, 0, to * n, n)[...] = (src[i * n:(i + 1) * n, pl.ds(pl.multiple_of(mine + c0, q), w)]
                                            + pre_s[at[k] + i * n:at[k] + (i + 1) * n, c0:c0 + w])
        n = n * 16
        h = n // 2
        flying[k] = [send(k, 0, 0, block(k, 0, 2, n), 0, h, 1), send(k, 0, 1, block(k, 0, 2, n, h), h, h, 3),
                     send(k, 0, 2, block(k, 0, 1, n, h), n + h, h, 1), send(k, 0, 3, block(k, 0, 3, n), 2 * n, h, 3)]

    def relay_first(k):
        n = shape[k][0] * 16
        h = n // 2
        for j, d, off, dst in ((0, 1, 0, n), (1, 3, h, 2 * n + h)):
            flying[k][j].wait_recv()
            to = acc_at(k, 0, block(k, 0, d, n, off), h)
            to[...] = to[...] + buf_at(k, 0, j * h, h)[...]
            flying[k].append(send(k, 0, 4 + j, block(k, 0, d, n, off), dst, h, d))

    def close_first(k):
        n = shape[k][0] * 16
        for c in flying[k][2:]:
            c.wait_recv()
        acc_at(k, 1, 0, n)[...] = acc_at(k, 0, block(k, 0, 0, n), n)[...] + (
            buf_at(k, 0, n, n)[...] + buf_at(k, 0, 2 * n, n)[...])
        flying[k] = launch(k, 1)

    open_first('c')
    for c in late:
        c.wait()
    wb = held(8)
    tg = dot_nt(lanes(wb, wb, wb), lanes(he_s[0:nt, :], he_s[nt:2 * nt, :], he_s[2 * nt:3 * nt, :]))
    norm_s[0:lat, 0:halo] = tg[:, 0:halo]
    norm_s[0:lat, halo:2 * halo] = tg[:, halo + band:nt]
    norm_s[lat:2 * lat, :] = tg[:, halo:halo + band]
    tails = [copy(norm_s.at[0:lat, 0:halo], pre_s.at[0:lat, 2 * halo:3 * halo], ts_sem.at[0], tr_sem.at[0], below),
             copy(norm_s.at[0:lat, halo:2 * halo], pre_s.at[0:lat, 3 * halo:4 * halo], ts_sem.at[1], tr_sem.at[1],
                  above)]
    started += tails
    open_first('a')
    open_first('b')

    gp, gn, ginv = grid_forward()
    keep_p, keep_n = slice(10 * lat, 11 * lat), slice(11 * lat, 12 * lat)
    norm_s[keep_p, :] = gp
    norm_s[keep_n, :] = gn
    inv_s[0] = ginv
    relay_first('c')
    relay_first('a')
    relay_first('b')
    own = cotg_s[...] + norm_s[lat:2 * lat, :]

    for c in tails:
        c.wait_recv()
    ends = lanes(own[:, 0:halo] + pre_s[0:lat, 3 * halo:4 * halo], own[:, halo:band - halo],
                 own[:, band - halo:band] + pre_s[0:lat, 2 * halo:3 * halo])
    gd = norm_back(ends * col(GRID, 2), norm_s[keep_n, :], inv_s[0])
    close_first('c')
    gg1 = grad_first(dot_nn(gw2_ref[...], gd.astype(BF)), norm_s[keep_p, :])
    ggrad_ref[...] = dot_nn(gw1_ref[...], gg1)
    close_first('a')
    close_first('b')

    for stage in (1, 2):
        for k in order:
            for c in flying[k]:
                c.wait_recv()
            n = shape[k][0] * 4 ** (2 - stage)
            acc_at(k, stage + 1, 0, n)[...] = (
                acc_at(k, stage, block(k, stage, 0, n), n)[...] + buf_at(k, stage, 0, n)[...]) + (
                buf_at(k, stage, n, n)[...] + buf_at(k, stage, 2 * n, n)[...])
            if stage < 2:
                flying[k] = launch(k, stage + 1)

    r1, r2 = o1_ref.shape[0], o2_ref.shape[0]
    win = r1 + r2
    f1, f2 = acc_rows['a'][3], acc_rows['c'][3]
    e1, e2 = top_b, top_b + win
    last = [copy(norm_s.at[pl.ds(pl.multiple_of(f1 + (1 - core) * 8, 8), win), 0:half], pre_s.at[e1:e1 + win, 0:half],
                 send4.at[0], recv4.at[0], partner),
            copy(norm_s.at[f2:f2 + b2, 0:half], pre_s.at[e2:e2 + b2, 0:half], send4.at[1], recv4.at[1], partner)]
    own1 = norm_s[pl.ds(pl.multiple_of(f1 + core * 8, 8), win), 0:half]
    own2 = norm_s[f2:f2 + b2, 0:half]
    low = core == 0
    o1_ref[:, pl.ds(mine, half)] = jnp.where(low, own1[0:r1], own1[r2:win])
    o2_ref[:, pl.ds(mine, half)] = jnp.where(low, own2[0:r2], own2[r2:b2])
    for c in last:
        c.wait_recv()
    got1 = pre_s[e1:e1 + win, 0:half]
    got2 = pre_s[e2:e2 + b2, 0:half]
    o1_ref[:, pl.ds(his, half)] = jnp.where(low, got1[0:r1], got1[r2:win])
    o2_ref[:, pl.ds(his, half)] = jnp.where(low, got2[0:r2], got2[r2:b2])
    for c in started + last:
        c.wait_send()


def finish_kernel(*refs):
    n = (len(refs) - 1) // 3
    bufs, sems = refs[2 * n:3 * n], refs[3 * n]
    ins = [pltpu.make_async_copy(refs[k], bufs[k], sems.at[0, k]) for k in range(n)]
    outs = [pltpu.make_async_copy(bufs[k], refs[n + k], sems.at[1, k]) for k in range(n)]
    for c in ins:
        c.start()
    for c, o in zip(ins, outs):
        c.wait()
        o.start()
    for o in outs:
        o.wait()


def finish_call(outs):
    n = len(outs)
    return pl.pallas_call(
        finish_kernel,
        out_shape=tuple(jax.ShapeDtypeStruct(o.shape, o.dtype) for o in outs),
        in_specs=[pl.BlockSpec(memory_space=pl.ANY)] * n,
        out_specs=(pl.BlockSpec(memory_space=pl.ANY),) * n,
        scratch_shapes=[VMEM(o.shape, o.dtype) for o in outs] + [pltpu.SemaphoreType.DMA((2, n))],
        compiler_params=pltpu.CompilerParams(vmem_limit_bytes=67043328),
        name='finish',
    )(*outs)


def step_call(args, sizes):
    band, nm, edges, lat, feats = sizes
    steps = edges // CHUNK
    nt = band + band // 2
    dma = pltpu.SemaphoreType.DMA
    out_shape = (jax.ShapeDtypeStruct((nm, lat), BF), jax.ShapeDtypeStruct((band, lat), BF),
                 jax.ShapeDtypeStruct((feats, band), F32), jax.ShapeDtypeStruct((3 * lat // 128, lat), F32),
                 jax.ShapeDtypeStruct((lat // 128, lat), F32))
    return pl.pallas_call(
        step_kernel,
        out_shape=out_shape,
        in_specs=[pl.BlockSpec(memory_space=pl.ANY if k in FETCHED else VMEM) for k in range(len(args))],
        out_specs=(pl.BlockSpec(memory_space=VMEM),) * len(out_shape),
        scratch_shapes=[VMEM((edges, CHUNK), F32), VMEM((edges, CHUNK), F32), VMEM((steps * lat, CHUNK), BF),
                        VMEM((steps, 1, CHUNK), F32), VMEM((lat, 2 * lat), BF), VMEM((lat, nm), F32),
                        VMEM((lat, nm), F32), VMEM((lat, CHUNK), BF), VMEM((lat, CHUNK), BF), VMEM((lat, CHUNK), BF),
                        VMEM((lat, band), F32),
                        VMEM((3 * lat, lat), F32), VMEM((lat, lat), F32), VMEM((lat, nt), BF),
                        VMEM((lat, nm), BF), VMEM((lat, lat), BF), VMEM((lat, lat), BF),
                        VMEM((lat, 128), F32), VMEM((lat, 7 * 128), F32), VMEM((lat, 4), BF),
                        dma((10,)), pltpu.SemaphoreType.REGULAR, dma((2,)), dma((2,)), dma((2,)), dma((2,)),
                        dma((5,)), dma((5,)), dma((3, 3, 6)), dma((3, 3, 6)), dma((2,)), dma((2,))],
        compiler_params=pltpu.CompilerParams(collective_id=0, has_side_effects=True, vmem_limit_bytes=67043328),
        name='whole_step',
    )(*args)


def solution(mesh):
    row_spec = P(('batch', 'graph'), None)
    flat_spec = P(('batch', 'graph'))
    rep_spec = P(None, None)

    def device_step(grid_in, mesh_in, edge_in, edge_src, edge_dst, edge_mask, *rest):
        sizes = (grid_in.shape[0], mesh_in.shape[0], edge_in.shape[0], rest[1].shape[1], grid_in.shape[1])
        args = (grid_in.T, mesh_in.T, edge_in.T, edge_src[None], edge_dst[None], edge_mask[None]) + rest
        mesh_out, grid_out, ggrad, w1_grad, w2_grad = finish_call(step_call(args, sizes))
        return mesh_out, grid_out, ggrad.T, w1_grad, w2_grad

    in_specs = (row_spec, row_spec, row_spec, flat_spec, flat_spec, flat_spec) + (rep_spec,) * 18 + (row_spec, row_spec)
    return jax.shard_map(device_step, mesh=mesh, in_specs=in_specs, out_specs=(row_spec,) * 5, check_vma=False)
```
